32 devices in a mesh: seq: 8 (over z, y), tp: 4 (over x, core).
Axes of the slice: x: 2, y: 2, z: 4, core: 2. Of those that a mesh axis runs over, the one named last changes fastest.
Arguments:
- tokens: bfloat16 [4096, 2048], P('seq'), may hold values from -16 to 16
- forget: float32 [4096, 32], P('seq', 'tp'), may hold values from -5 to 0, as said below
- attn_gain: float32 [2048], replicated, may hold values from 0.1 to 1.9
- projections: bfloat16 [3, 2048, 2048], P(None, None, 'tp'), may hold values from -0.125 to 0.125
- out_weight: bfloat16 [2048, 2048], P('tp'), may hold values from -0.125 to 0.125
- ffn_gain: float32 [2048], replicated, may hold values from 0.1 to 1.9
- expand_weight: bfloat16 [2, 2048, 4096], P(None, None, 'tp'), may hold values from -0.125 to 0.125
- down_weight: bfloat16 [4096, 2048], P('tp'), may hold values from -0.09375 to 0.09375
Outputs:
- output: bfloat16 [4096, 2048], P('seq')
The draws below stay inside these ranges and needn't reach their ends.
Inputs may be any that keep to these rules, and one draw needn't show every extreme that they name: forget is never positive.
All inputs are finite; a program needn't handle non-finite values.
Results may differ from the reference program's by a relative error of at most 0.011.
Values may be sent and summed in bfloat16 or wider, within the bound.
A program may use at most 128 MiB of HBM per device.

```python
import math
import jax
import jax.numpy as jnp
from jax import lax

D = 2048
HEAD_TOTAL = 32
DH = 64
FF = 4096
TOK_DEV = 512
SEQUENCE_TOKENS = 4096


def draw_tokens(key, part):
    random_keys = jax.random.split(key, 3)
    noise = jax.random.normal(random_keys[0], (SEQUENCE_TOKENS, D), jnp.float32)
    row_scale = jnp.exp(jax.random.uniform(random_keys[1], (SEQUENCE_TOKENS, 1), jnp.float32, jnp.log(0.3), jnp.log(3.0)))
    column_scale = jnp.exp(jax.random.uniform(random_keys[2], (1, D), jnp.float32, jnp.log(0.3), jnp.log(3.0)))
    return jnp.clip(noise * row_scale * column_scale, -16.0, 16.0).astype(jnp.bfloat16)


def draw_forget(key, part):
    random_keys = jax.random.split(key, 7)
    slow_share = 0.5
    is_slow = jax.random.uniform(random_keys[0], (HEAD_TOTAL,), jnp.float32) < slow_share
    slow_rate = jax.random.uniform(random_keys[1], (HEAD_TOTAL,), jnp.float32, 0.2, 0.6) / SEQUENCE_TOKENS
    fast_rate = jnp.exp(jax.random.uniform(random_keys[2], (HEAD_TOTAL,), jnp.float32, jnp.log(10.0), jnp.log(16.0))) / TOK_DEV
    base_rate = jnp.where(is_slow, slow_rate, fast_rate)
    block_count = SEQUENCE_TOKENS // TOK_DEV
    device_factor = jnp.exp(jax.random.uniform(random_keys[3], (block_count, 1, HEAD_TOTAL), jnp.float32, jnp.log(0.5), jnp.log(2.0)))
    roughness = jax.random.uniform(random_keys[4], (block_count, TOK_DEV, HEAD_TOTAL), jnp.float32, 0.5, 1.5)
    decay_rates = (base_rate * device_factor * roughness).reshape(SEQUENCE_TOKENS, HEAD_TOTAL)
    spike_positions = jax.random.randint(random_keys[5], (2,), 0, SEQUENCE_TOKENS)
    spike_magnitude = jax.random.uniform(random_keys[6], (2, HEAD_TOTAL), jnp.float32, 0.22, 0.69)
    spike_flags = (jnp.arange(SEQUENCE_TOKENS)[:, None] == spike_positions[None, :]).astype(jnp.float32)
    spike_values = jnp.dot(spike_flags, spike_magnitude)
    return -(decay_rates + spike_values)


def block_scale(key, extent, shards, least, top_value):
    factor_of, own = 1.0, jax.random.fold_in(key, 6)
    for axis_at, blocks in shards:
        draws = jnp.exp(jax.random.uniform(jax.random.fold_in(own, axis_at), (blocks,), jnp.float32, least / len(shards), top_value / len(shards)))
        factor_of = factor_of * jnp.repeat(draws, extent[axis_at] // blocks).reshape([-1 if axis == axis_at else 1 for axis in range(len(extent))])
    return factor_of


def gaussian(stream_key, shape, width, reach, shards=(), dtype=jnp.bfloat16):
    entries = width * jax.random.normal(stream_key, shape, jnp.float32)
    if shards:
        entries = entries * block_scale(stream_key, shape, shards, -0.22, 0.18)
    return jnp.clip(entries, -reach, reach).astype(dtype)


def setup_inputs(seed: int = 0) -> dict:
    splits = jax.random.split(jax.random.key(seed), 9)
    tokens = draw_tokens(jax.random.fold_in(splits[8], 71), 0)
    forget = draw_forget(jax.random.fold_in(splits[8], 71), 0)
    attn_gain = jnp.clip(1.0 + 0.18 * jax.random.normal(splits[2], (D,), jnp.float32), 0.1, 1.9)
    projections = gaussian(splits[3], (3, D, HEAD_TOTAL * DH), D ** -0.5, 0.125, ((2, 4),))
    out_weight = gaussian(splits[4], (HEAD_TOTAL * DH, D), (HEAD_TOTAL * DH) ** -0.5, 0.125, ((0, 4),))
    ffn_gain = jnp.clip(1.0 + 0.18 * jax.random.normal(splits[5], (D,), jnp.float32), 0.1, 1.9)
    expand_weight = gaussian(splits[6], (2, D, FF), D ** -0.5, 0.125, ((2, 4),))
    down_weight = gaussian(splits[7], (FF, D), FF ** -0.5, 0.09375, ((0, 4),))
    return dict(tokens=tokens, forget=forget, attn_gain=attn_gain, projections=projections, out_weight=out_weight, ffn_gain=ffn_gain, expand_weight=expand_weight, down_weight=down_weight)


norm_epsilon = 1e-05
head_epsilon = 1e-06

def rms_scale(values, gain_vector):
    widened = values.astype(jnp.float32)
    mean_square = lax.optimization_barrier(jnp.mean(widened * widened, axis=-1, keepdims=True))
    return widened * lax.rsqrt(mean_square + norm_epsilon) * gain_vector

def summarize(key_rows, value_rows, forget_rows):
    log_decay = jnp.cumsum(forget_rows, axis=0)
    block_total = log_decay[-1]
    shrink_factors = jnp.exp(block_total[None, :] - log_decay)
    scaled_keys = (key_rows.astype(jnp.float32) * shrink_factors[:, :, None]).astype(jnp.bfloat16)
    block_state = jnp.einsum('shd,she->hde', scaled_keys.astype(jnp.float32), value_rows.astype(jnp.float32), precision=lax.Precision.HIGHEST)
    return (log_decay, block_total, block_state)

def attend_local(query_rows, key_rows, value_rows, log_decay, incoming):
    head_size = query_rows.shape[2]
    score_scale = 1.0 / math.sqrt(head_size)
    query_wide = query_rows.astype(jnp.float32)
    scores = jnp.einsum('thd,shd->hts', query_wide, key_rows.astype(jnp.float32), precision=lax.Precision.HIGHEST) * score_scale
    log_gaps = log_decay.T[:, :, None] - log_decay.T[:, None, :]
    row_order = jnp.arange(query_rows.shape[0])
    causal = (row_order[:, None] >= row_order[None, :])[None]
    local_weights = jnp.where(causal, scores * jnp.exp(jnp.where(causal, log_gaps, 0.0)), 0.0).astype(jnp.bfloat16)
    local_part = jnp.einsum('hts,she->the', local_weights.astype(jnp.float32), value_rows.astype(jnp.float32), precision=lax.Precision.HIGHEST)
    carried = jnp.einsum('thd,hde->the', query_wide, incoming, precision=lax.Precision.HIGHEST)
    attended = local_part + carried * (jnp.exp(log_decay) * score_scale)[:, :, None]
    mean_square = lax.optimization_barrier(jnp.mean(attended * attended, axis=-1, keepdims=True))
    return (attended * lax.rsqrt(mean_square + head_epsilon)).astype(jnp.bfloat16)

def reference(tokens, forget, attn_gain, projections, out_weight, ffn_gain, expand_weight, down_weight):
    normed = rms_scale(tokens, attn_gain).astype(jnp.bfloat16)
    block_count = SEQUENCE_TOKENS // TOK_DEV
    shaped = []
    for which in range(3):
        projected = jnp.dot(normed, projections[which], preferred_element_type=jnp.float32).astype(jnp.bfloat16)
        shaped.append(projected.reshape(block_count, TOK_DEV, HEAD_TOTAL, DH))
    forget_blocks = forget.reshape(block_count, TOK_DEV, HEAD_TOTAL)

    def block_step(incoming, block_data):
        query_rows, key_rows, value_rows, forget_rows = block_data
        log_decay, block_total, block_state = summarize(key_rows, value_rows, forget_rows)
        head_out = attend_local(query_rows, key_rows, value_rows, log_decay, incoming)
        following = jnp.exp(block_total)[:, None, None] * incoming + block_state
        return (following, head_out)
    start_state = jnp.zeros((HEAD_TOTAL, DH, DH), jnp.float32)
    _, head_blocks = lax.scan(block_step, start_state, (shaped[0], shaped[1], shaped[2], forget_blocks))
    head_out = head_blocks.reshape(SEQUENCE_TOKENS, HEAD_TOTAL * DH)
    attn_out = jnp.dot(head_out, out_weight, preferred_element_type=jnp.float32)
    residual = (tokens.astype(jnp.float32) + attn_out).astype(jnp.bfloat16)
    normed_ffn = rms_scale(residual, ffn_gain).astype(jnp.bfloat16)
    gate_proj = jnp.dot(normed_ffn, expand_weight[0], preferred_element_type=jnp.float32)
    up_proj = jnp.dot(normed_ffn, expand_weight[1], preferred_element_type=jnp.float32)
    hidden = (jax.nn.silu(gate_proj) * up_proj).astype(jnp.bfloat16)
    ffn_out = jnp.dot(hidden, down_weight, preferred_element_type=jnp.float32)
    return (residual.astype(jnp.float32) + ffn_out).astype(jnp.bfloat16)
```

```python
import functools

import jax
import jax.numpy as jnp
from jax import lax
from jax.experimental import pallas as pl
from jax.experimental.pallas import tpu as pltpu
from jax.sharding import PartitionSpec as P

norm_epsilon = 1e-05
head_epsilon = 1e-06
MESH = pl.DeviceIdType.MESH
CHUNKS = 4
SIZES = (2, 2, 2, 2)
PLAIN = 1
SUB = 8
VIA_Z = ()
VIA_Y = (0, 1, 2, 3, 4)
STRAIGHT = (5, 6, 7)
F32 = jnp.float32
BF16 = jnp.bfloat16


def dot(a, b):
    return jnp.dot(a, b, preferred_element_type=F32)


def contract(a, b, dim_a, dim_b):
    return lax.dot_general(
        a, b, (((dim_a,), (dim_b,)), ((), ())), preferred_element_type=F32
    )


def normalize(widened, gain):
    mean_square = jnp.mean(widened * widened, axis=-1, keepdims=True)
    return (widened * lax.rsqrt(mean_square + norm_epsilon) * gain).astype(BF16)


def kernel(
    blocks, steps,
    tok_hbm, fgt, again, proj_hbm, ow_hbm, fgain, ew_hbm, dw_hbm,
    out,
    tok, wq, wk, wv, wo, wg, wu, wd,
    normed, q, k, v, att, ho, bd, es, el, ts, tl, ed, td, tsb, tsl, trb, trl,
    part, own, dsend1, drecv1, xsend1, xrecv1, nf, res, hid,
    dsend2, drecv2, xsend2, xrecv2,
    ks, ld, ldt,
    wsem, tsem, sts, strv, wxs, wxr, wys, wyr, wzs, wzr, wcs, wcr,
    d1s, d1r, x1s, x1r, hs, hr, ns, nr, d2s, d2r, x2s, x2r, osd, orv,
):
    rows, width = tok.shape
    heads = fgt.shape[0]
    inner = wk.shape[1]
    pairs = heads // 2
    chunk = rows // CHUNKS
    me = lax.axis_index("seq")
    tp = lax.axis_index("tp")
    core = lax.rem(tp, 2)
    side = lax.div(tp, 2)
    partner = tp + 1 - 2 * core
    across = lax.rem(tp + 2, 4)
    place = lax.rem(me, 4)
    bit_y = lax.rem(me, 2)
    bit_z = lax.div(place, 2)
    next_y = me + 1 - 2 * bit_y
    next_z = me + 2 - 4 * bit_z

    loads = []
    for at, (src, dst) in enumerate((
        (proj_hbm.at[1], wk), (proj_hbm.at[2], wv), (proj_hbm.at[0], wq),
        (ow_hbm, wo.at[side]), (ew_hbm.at[0], wg), (ew_hbm.at[1], wu), (dw_hbm, wd),
    )):
        copy = pltpu.make_async_copy(src, dst, wsem.at[at])
        loads.append(copy)
    def token_load(r):
        at = pl.ds(pl.multiple_of(r * chunk, chunk), chunk)
        return pltpu.make_async_copy(tok_hbm.at[at], tok.at[at], tsem.at[r])

    for r in range(CHUNKS):
        token_load(r).start()

    barrier = pltpu.get_barrier_semaphore()
    for other in (partner, across):
        pl.semaphore_signal(barrier, inc=1, device_id={"tp": other}, device_id_type=MESH)
    for other in (next_y, next_z):
        pl.semaphore_signal(barrier, inc=1, device_id={"seq": other}, device_id_type=MESH)
    for step in range(1, steps):
        for far in (2 ** step, blocks - 2 ** step):
            pl.semaphore_signal(
                barrier, inc=1, device_id={"seq": lax.rem(me + far, blocks)}, device_id_type=MESH)

    quarter = inner // 4
    sub = quarter // SUB

    def strip(owner, j):
        return pl.ds(pl.multiple_of(owner * quarter + j * sub, sub), sub)

    def on_seq(src, dst, ssem, rsem, other):
        return pltpu.make_async_remote_copy(
            src, dst, ssem, rsem, device_id={"seq": other}, device_id_type=MESH)

    def to(src, dst, ssem, rsem, other):
        return pltpu.make_async_remote_copy(
            src, dst, ssem, rsem, device_id={"tp": other}, device_id_type=MESH)

    far_wo = wo.at[1 - side]
    place_y = place + 1 - 2 * bit_y
    place_z = place + 2 - 4 * bit_z

    def wx(j):
        return to(ow_hbm.at[strip(place, j)], wo.at[side, strip(place, j)], wxs.at[j], wxr.at[j], across)

    def wy(j):
        at = strip(place, j)
        return on_seq(far_wo.at[at], far_wo.at[at], wys.at[j], wyr.at[j], next_y)

    def wz(j):
        at = strip(place, j)
        return on_seq(far_wo.at[at], far_wo.at[at], wzs.at[j], wzr.at[j], next_z)

    def wc(j):
        at = strip(3 - place, j)
        return to(ow_hbm.at[at], wo.at[side, at], wcs.at[j], wcr.at[j], across)

    def corner(j):
        if j in VIA_Z:
            at = strip(place_y, j)
            return on_seq(far_wo.at[at], far_wo.at[at], wcs.at[j], wcr.at[j], next_z)
        at = strip(place_z, j)
        return on_seq(far_wo.at[at], far_wo.at[at], wcs.at[j], wcr.at[j], next_y)

    def pass_y(j):
        wx(j).wait_recv()
        wy(j).start()

    def pass_z(j):
        wz(j).start()

    def pass_corner(j):
        if j in VIA_Z:
            wy(j).wait_recv()
        else:
            wz(j).wait_recv()
        corner(j).start()

    runs = rows // 128
    tri = (
        lax.broadcasted_iota(jnp.int32, (128, 128), 0)
        <= lax.broadcasted_iota(jnp.int32, (128, 128), 1)
    ).astype(F32).astype(BF16)
    rounded = []
    for b in range(runs):
        left = fgt[:, 128 * b : 128 * b + 128]
        for _ in range(3):
            top = left.astype(BF16).astype(F32)
            rounded.append(top)
            left = left - top
    sums = dot(jnp.concatenate(rounded, axis=0).astype(BF16), tri)
    carried = jnp.zeros((heads, 1), F32)
    for b in range(runs):
        at = 3 * heads * b
        run = sums[at : at + heads] + sums[at + heads : at + 2 * heads]
        run = run + sums[at + 2 * heads : at + 3 * heads] + carried
        ldt[:, 128 * b : 128 * b + 128] = run
        ld[128 * b : 128 * b + 128, :] = run.T
        carried = run[:, 127:128]
    loads[0].start()
    pl.semaphore_wait(barrier, 4 + 2 * (steps - 1))
    for j in range(SUB):
        wx(j).start()
    for j in STRAIGHT:
        wc(j).start()


    def norm_chunk(r, carry):
        at = pl.ds(pl.multiple_of(r * chunk, chunk), chunk)
        token_load(r).wait()
        normed[at, :] = normalize(tok[at, :].astype(F32), again[...])
        return carry

    loads[1].start()
    lax.fori_loop(0, CHUNKS, norm_chunk, 0)

    def project(weight, dst):
        tile = min(256, dst.shape[1])

        def body(j, carry):
            at = pl.ds(pl.multiple_of(j * tile, tile), tile)
            dst[:, at] = dot(normed[...], weight[:, at]).astype(BF16)
            return carry

        lax.fori_loop(0, dst.shape[1] // tile, body, 0)

    loads[2].start()
    loads[3].start()
    loads[0].wait()
    project(wk, k)
    loads[1].wait()

    low = lax.broadcasted_iota(jnp.int32, (1, 128), 1) < 64
    low_f = low.astype(F32)
    masks_f = (low_f, 1.0 - low_f)
    masks = (masks_f[0].astype(BF16), masks_f[1].astype(BF16))

    def spread(columns, p):
        return jnp.where(low, columns[:, 2 * p : 2 * p + 1], columns[:, 2 * p + 1 : 2 * p + 2])

    log_decay = ld[...]
    last = log_decay[rows - 1 : rows, :]
    shrink = jnp.exp(ldt[:, rows - 1 : rows] - ldt[...])
    tl[...] = jnp.zeros_like(tl)
    el[...] = jnp.zeros_like(el)
    es[...] = jnp.zeros_like(es)
    for p in range(pairs):
        tl[p : p + 1, :] = spread(last, p)
    part_pairs = pairs // 2

    later = bit_y == 1

    def heir(step):
        return me + 2 ** step if step else next_y

    def sends(step):
        return me + 2 ** step < blocks if step else me >= 0

    def takes(step):
        return me >= 2 ** step if step else me >= 0

    def state_copy(step, part_of):
        at = slice(64 * part_pairs * part_of, 64 * part_pairs * (part_of + 1))
        return pltpu.make_async_remote_copy(
            tsb.at[step, at], trb.at[step, at], sts.at[step, part_of], strv.at[step, part_of],
            device_id={"seq": heir(step)}, device_id_type=MESH)

    def decay_copy(step):
        return pltpu.make_async_remote_copy(
            tsl.at[step], trl.at[step], sts.at[step, 2], strv.at[step, 2],
            device_id={"seq": heir(step)}, device_id_type=MESH)

    def state_copies(step):
        return (decay_copy(step), state_copy(step, 0), state_copy(step, 1))

    def send_state(step, part_of):
        @pl.when(sends(step))
        def _():
            at = slice(64 * part_pairs * part_of, 64 * part_pairs * (part_of + 1))
            if part_of == 0:
                tsl[step] = tl[...]
                decay_copy(step).start()
            tsb[step, at, :] = ts[at, :].astype(BF16)
            state_copy(step, part_of).start()

    def take_state(step):
        for part_of in range(2):
            @pl.when(takes(step))
            def _():
                if part_of == 0:
                    decay_copy(step).wait_recv()
                    ed[...] = jnp.exp(el[...])
                    td[...] = jnp.exp(tl[...])
                    if step == 0:
                        td[...] = jnp.where(later, td[...], jnp.exp(trl[step]))
                        el[...] = jnp.where(later, trl[step], el[...])
                    else:
                        el[...] = el[...] + trl[step]
                    tl[...] = tl[...] + trl[step]
                state_copy(step, part_of).wait_recv()
                for p in range(part_pairs * part_of, part_pairs * (part_of + 1)):
                    at = slice(64 * p, 64 * p + 64)
                    came = trb[step, at, :].astype(F32)
                    decay = td[p : p + 1, :]
                    if step == 0:
                        mine_first = ts[at, :]
                        es[at, :] = jnp.where(later, came, 0.0)
                        ts[at, :] = jnp.where(
                            later, mine_first + decay * came, decay * mine_first + came)
                    else:
                        es[at, :] = es[at, :] + ed[p : p + 1, :] * came
                        ts[at, :] = ts[at, :] + decay * came

            if step + 1 < steps:
                send_state(step + 1, part_of)

    for p in range(pairs):
        turned = k[:, 128 * p : 128 * p + 128].T.astype(F32)
        for j in range(2):
            h = 2 * p + j
            ks[64 * h : 64 * h + 64, :] = (turned[64 * j : 64 * j + 64] * shrink[h : h + 1, :]).astype(BF16)
    each = 128 * part_pairs
    for part_of in range(2):
        cols = slice(each * part_of, each * (part_of + 1))
        v[:, cols] = dot(normed[...], wv[:, cols]).astype(BF16)
        state = dot(ks[cols, :], v[:, cols])
        for p in range(part_pairs):
            at = slice(128 * p, 128 * p + 128)
            pair = state[at, at]
            h = 64 * (part_pairs * part_of + p)
            ts[h : h + 64, :] = pair[:64] * masks_f[0] + pair[64:] * masks_f[1]
        if steps:
            send_state(0, part_of)

    for at in (4, 5, 6):
        loads[at].start()
    loads[2].wait()
    project(wq, q)

    span = rows // 2
    taken = 0
    for p in range(pairs):
        lanes = slice(128 * p, 128 * p + 128)
        for piece in range(2):
            at = slice(piece * span, piece * span + span)
            reach = (piece + 1) * span
            causal = (
                lax.broadcasted_iota(jnp.int32, (span, reach), 0) + piece * span
                >= lax.broadcasted_iota(jnp.int32, (span, reach), 1)
            )
            sums = []
            for j in range(2):
                h = 2 * p + j
                scores = contract(q[at, lanes] * masks[j], k[:reach, lanes], 1, 1)
                gaps = jnp.where(causal, ld[at, h : h + 1] - ldt[h : h + 1, :reach], -1e30)
                weights = (scores * 0.125 * jnp.exp(gaps)).astype(BF16)
                sums.append(dot(weights, v[:reach, lanes]))
            att[at, lanes] = jnp.where(low, sums[0], sums[1])
            if p % 2 == 0 and piece and taken < steps:
                take_state(taken)
                taken += 1
                if taken == 1:
                    for j in range(3):
                        pass_y(j)
        if p == pairs - 2:
            pass_y(3)
    for j in (4, 5):
        pass_y(j)
    while taken < steps:
        take_state(taken)
        taken += 1

    for j in range(6, SUB):
        pass_y(j)
    for j in range(SUB):
        pass_z(j)

    for p in range(pairs):
        came = es[64 * p : 64 * p + 64, :]
        bd[p] = jnp.concatenate([came * masks_f[0], came * masks_f[1]], axis=0).astype(BF16)
    same_head = (
        (lax.broadcasted_iota(jnp.int32, (128, 128), 0) < 64)
        == (lax.broadcasted_iota(jnp.int32, (128, 128), 1) < 64)
    ).astype(F32).astype(BF16)

    starts, total = [], 0
    for size in SIZES:
        starts.append(total * (rows // sum(SIZES)))
        total += size
    sizes = [size * (rows // sum(SIZES)) for size in SIZES]
    count = len(sizes)

    def whole_rows(r):
        return slice(starts[r], starts[r] + sizes[r])

    def half_rows(r):
        return slice(starts[r] // 2, starts[r] // 2 + sizes[r] // 2)

    def own_rows(r):
        half = sizes[r] // 2
        return pl.ds(pl.multiple_of(starts[r] + core * half, half), half)

    def mine(r):
        half = sizes[r] // 2
        return pl.ds(pl.multiple_of(core * half, half), half)

    def theirs(r):
        half = sizes[r] // 2
        return pl.ds(pl.multiple_of(half - core * half, half), half)

    def d1(r):
        at = half_rows(r)
        return to(dsend1.at[at], drecv1.at[at], d1s.at[r], d1r.at[r], partner)

    def x1(r):
        at = half_rows(r)
        return to(xsend1.at[at], xrecv1.at[at], x1s.at[r], x1r.at[r], across)

    def hx(r):
        at = whole_rows(r)
        return to(ho.at[side, at], ho.at[side, at], hs.at[r], hr.at[r], across)

    def nfc(r):
        return to(nf.at[own_rows(r)], nf.at[own_rows(r)], ns.at[r], nr.at[r], partner)

    def d2(r):
        at = half_rows(r)
        return to(dsend2.at[at], drecv2.at[at], d2s.at[r], d2r.at[r], partner)

    def x2(r, piece):
        n = sizes[r] // 4
        at = pl.ds(starts[r] // 2 + piece * n, n)
        return to(xsend2.at[at], xrecv2.at[at], x2s.at[r, piece], x2r.at[r, piece], across)

    def oc(r, piece):
        at = out_rows(r, piece)
        return to(out.at[at], out.at[at], osd.at[r, piece], orv.at[r, piece], partner)

    def out_rows(r, piece):
        n = sizes[r] // 4
        return pl.ds(pl.multiple_of(starts[r] + core * 2 * n + piece * n, n), n)

    loads[3].wait()
    wide = min(512, width)

    def attend(r):
        at = whole_rows(r)
        reach_decay = jnp.exp(ld[at, :]) * 0.125
        for p in range(pairs):
            lanes = slice(128 * p, 128 * p + 128)
            attended = att[at, lanes] + dot(q[at, lanes], bd[p]) * spread(reach_decay, p)
            mean_square = dot((attended * attended).astype(BF16), same_head) * (1.0 / 64)
            ho[side, at, lanes] = (attended * lax.rsqrt(mean_square + head_epsilon)).astype(BF16)

    def halve(r, send, copy):
        n = sizes[r]
        own[half_rows(r), :] = part[mine(r), :]
        send[half_rows(r), :] = part[theirs(r), :].astype(BF16)
        copy.start()

    def combine(r):
        at, n = whole_rows(r), sizes[r]
        for c in range(width // wide):
            cols = slice(c * wide, c * wide + wide)
            if r < PLAIN:
                part[:n, cols] = dot(ho[side, at, :], wo[side, :, cols])
            else:
                part[:n, cols] = dot(ho[0, at, :], wo[0, :, cols]) + dot(ho[1, at, :], wo[1, :, cols])
        halve(r, dsend1, d1(r))

    def cross(r):
        at = half_rows(r)
        d1(r).wait_recv()
        xsend1[at, :] = (own[at, :] + drecv1[at, :].astype(F32)).astype(BF16)
        x1(r).start()

    def settle(r):
        at = half_rows(r)
        if r < PLAIN:
            x1(r).wait_recv()
            added = xsend1[at, :].astype(F32) + xrecv1[at, :].astype(F32)
        else:
            d1(r).wait_recv()
            added = own[at, :] + drecv1[at, :].astype(F32)
        kept = (tok[own_rows(r), :].astype(F32) + added).astype(BF16)
        res[at, :] = kept
        nf[own_rows(r), :] = normalize(kept.astype(F32), fgain[...])
        nfc(r).start()

    hidden_width = wg.shape[1]
    tile = min(256, hidden_width)

    def forward(r):
        nfc(r).wait_recv()
        at, n = whole_rows(r), sizes[r]
        for c in range(hidden_width // tile):
            cols = slice(c * tile, c * tile + tile)
            gate = dot(nf[at, :], wg[:, cols])
            up = dot(nf[at, :], wu[:, cols])
            hid[:n, cols] = (gate / (1.0 + jnp.exp(-gate)) * up).astype(BF16)
        for c in range(width // wide):
            cols = slice(c * wide, c * wide + wide)
            part[:n, cols] = dot(hid[:n, :], wd[:, cols])
        halve(r, dsend2, d2(r))

    def pass_sums(r):
        at = half_rows(r)
        d2(r).wait_recv()
        xsend2[at, :] = (own[at, :] + drecv2[at, :].astype(F32)).astype(BF16)
        x2(r, 0).start()
        x2(r, 1).start()

    def finish(r, piece):
        n = sizes[r] // 4
        at = slice(starts[r] // 2 + piece * n, starts[r] // 2 + piece * n + n)
        x2(r, piece).wait_recv()
        added = xsend2[at, :].astype(F32) + xrecv2[at, :].astype(F32)
        out[out_rows(r, piece), :] = (res[at, :].astype(F32) + added).astype(BF16)
        oc(r, piece).start()

    if PLAIN < count:
        attend(PLAIN)
        hx(PLAIN).start()
    for r in range(PLAIN):
        attend(r)
        combine(r)
    for r in range(PLAIN + 1, count):
        attend(r)
    for r in range(PLAIN):
        cross(r)
    for r in range(PLAIN + 1, count):
        hx(r).start()
    for at in (4, 5, 6):
        loads[at].wait()

    def arrive():
        for j in range(SUB):
            if j not in VIA_Z:
                wy(j).wait_recv()
            if j not in VIA_Y:
                wz(j).wait_recv()
            if j in STRAIGHT:
                wc(j).wait_recv()
            else:
                corner(j).wait_recv()

    def combine_late(r):
        if r == PLAIN:
            arrive()
        hx(r).wait_recv()
        combine(r)

    for j in VIA_Z + VIA_Y:
        pass_corner(j)
    settle(0)
    for r in range(count):
        if PLAIN < r + 1 < count:
            combine_late(r + 1)
        if r > PLAIN:
            pass_sums(r - 1)
        forward(r)
        if r + 1 == PLAIN < count:
            combine_late(r + 1)
        if r < PLAIN:
            pass_sums(r)
        if r + 1 < count:
            settle(r + 1)
    pass_sums(count - 1)
    for j in range(SUB):
        for copy in (wx(j), wy(j), wz(j), wc(j) if j in STRAIGHT else corner(j)):
            copy.wait_send()
    for step in range(steps):
        @pl.when(sends(step))
        def _():
            for copy in state_copies(step):
                copy.wait_send()
    for r in range(count):
        for copy in (d1(r), nfc(r), d2(r), x1(r) if r < PLAIN else hx(r)):
            copy.wait_send()
    for r in range(count):
        for piece in range(2):
            finish(r, piece)
    for r in range(count):
        for piece in range(2):
            x2(r, piece).wait_send()
            oc(r, piece).wait()


def local(blocks, tokens, forget, attn_gain, projections, out_weight, ffn_gain, expand_weight, down_weight):
    rows, width = tokens.shape
    heads = forget.shape[1]
    inner = projections.shape[2]
    hidden = down_weight.shape[0]
    pairs = heads // 2
    steps = max(blocks - 1, 0).bit_length()
    V = pltpu.VMEM
    S = pltpu.SemaphoreType.DMA
    slots = max(steps, 1)
    count = len(SIZES)
    largest = rows // sum(SIZES) * max(SIZES)
    halves = V((rows // 2, width), BF16)
    early = V((rows // sum(SIZES) * sum(SIZES[:max(PLAIN, 1)]) // 2, width), BF16)
    scratch = [
        V((rows, width), BF16),
        V((width, inner), BF16), V((width, inner), BF16), V((width, inner), BF16),
        V((2, inner, width), BF16),
        V((width, hidden), BF16), V((width, hidden), BF16), V((hidden, width), BF16),
        V((rows, width), BF16),
        V((rows, inner), BF16), V((rows, inner), BF16), V((rows, inner), BF16),
        V((rows, inner), F32), V((2, rows, inner), BF16),
        V((pairs, 128, 128), BF16),
        V((64 * pairs, 128), F32), V((8, 128), F32), V((64 * pairs, 128), F32), V((8, 128), F32),
        V((8, 128), F32), V((8, 128), F32),
        V((slots, 64 * pairs, 128), BF16), V((slots, 8, 128), F32),
        V((slots, 64 * pairs, 128), BF16), V((slots, 8, 128), F32),
        V((largest, width), F32), V((rows // 2, width), F32),
        halves, halves, early, early,
        V((rows, width), BF16), halves, V((largest, hidden), BF16),
        halves, halves, halves, halves,
        V((inner, rows), BF16), V((rows, heads), F32), V((heads, rows), F32),
        S((8,)), S((CHUNKS,)), S((slots, 3)), S((slots, 3)),
    ] + [S((SUB,)) for _ in range(8)] + [S((count,)) for _ in range(10)] + [S((count, 2)) for _ in range(4)]
    hbm = pl.BlockSpec(memory_space=pl.ANY)
    vmem = pl.BlockSpec(memory_space=pltpu.VMEM)
    return pl.pallas_call(
        functools.partial(kernel, blocks, steps),
        out_shape=pltpu.VMEM((rows, width), BF16),
        in_specs=[hbm, vmem, vmem, hbm, hbm, vmem, hbm, hbm],
        out_specs=vmem,
        scratch_shapes=scratch,
        compiler_params=pltpu.CompilerParams(
            collective_id=0, has_side_effects=True, vmem_limit_bytes=60_000_000
        ),
    )(
        tokens, forget.T, attn_gain[None, :], projections, out_weight,
        ffn_gain[None, :], expand_weight, down_weight,
    )


def solution(mesh):
    placed = (
        P("seq", None),
        P("seq", "tp"),
        P(),
        P(None, None, "tp"),
        P("tp", None),
        P(),
        P(None, None, "tp"),
        P("tp", None),
    )
    return jax.shard_map(
        functools.partial(local, mesh.shape["seq"]),
        mesh=mesh, in_specs=placed, out_specs=P("seq", None), check_vma=False,
    )
```

```python
import functools

import jax
import jax.numpy as jnp
from jax import lax
from jax.experimental import pallas as pl
from jax.experimental.pallas import tpu as pltpu
from jax.sharding import PartitionSpec as P

norm_epsilon = 1e-05
head_epsilon = 1e-06
MESH = pl.DeviceIdType.MESH
CHUNKS = 4
SIZES = (2, 2, 2, 2)
PLAIN = 1
SUB = 8
VIA_Z = (0,)
VIA_Y = (1, 2, 3, 4, 5)
STRAIGHT = (6, 7)
F32 = jnp.float32
BF16 = jnp.bfloat16


def dot(a, b):
    return jnp.dot(a, b, preferred_element_type=F32)


def contract(a, b, dim_a, dim_b):
    return lax.dot_general(
        a, b, (((dim_a,), (dim_b,)), ((), ())), preferred_element_type=F32
    )


def normalize(widened, gain):
    mean_square = jnp.mean(widened * widened, axis=-1, keepdims=True)
    return (widened * lax.rsqrt(mean_square + norm_epsilon) * gain).astype(BF16)


def kernel(
    blocks, steps,
    tok_hbm, fgt_hbm, again_hbm, proj_hbm, ow_hbm, fgain_hbm, ew_hbm, dw_hbm,
    out,
    fgt, again, fgain,
    tok, wq, wk, wv, wo, wg, wu, wd,
    normed, q, k, v, att, ho, bd, es, el, ts, tl, ed, td, tsb, tsl, trb, trl,
    part, own, dsend1, drecv1, xsend1, xrecv1, nf, res, hid,
    dsend2, drecv2, xsend2, xrecv2,
    ks, ld, ldt,
    wsem, tsem, small_sem, sts, strv, wxs, wxr, wys, wyr, wzs, wzr, wcs, wcr,
    d1s, d1r, x1s, x1r, hs, hr, ns, nr, d2s, d2r, x2s, x2r, osd, orv,
):
    rows, width = tok.shape
    heads = fgt.shape[0]
    inner = wk.shape[1]
    pairs = heads // 2
    chunk = rows // CHUNKS
    me = lax.axis_index("seq")
    tp = lax.axis_index("tp")
    core = lax.rem(tp, 2)
    side = lax.div(tp, 2)
    partner = tp + 1 - 2 * core
    across = lax.rem(tp + 2, 4)
    place = lax.rem(me, 4)
    bit_y = lax.rem(me, 2)
    bit_z = lax.div(place, 2)
    next_y = me + 1 - 2 * bit_y
    next_z = me + 2 - 4 * bit_z

    loads = []
    for at, (src, dst) in enumerate((
        (proj_hbm.at[1], wk), (proj_hbm.at[2], wv), (proj_hbm.at[0], wq),
        (ow_hbm, wo.at[side]), (ew_hbm.at[0], wg), (ew_hbm.at[1], wu), (dw_hbm, wd),
    )):
        copy = pltpu.make_async_copy(src, dst, wsem.at[at])
        loads.append(copy)
    def token_load(r):
        at = pl.ds(pl.multiple_of(r * chunk, chunk), chunk)
        return pltpu.make_async_copy(tok_hbm.at[at], tok.at[at], tsem.at[r])

    small = []
    for at, (src, dst) in enumerate(((fgt_hbm, fgt), (again_hbm, again), (fgain_hbm, fgain))):
        small.append(pltpu.make_async_copy(src, dst, small_sem.at[at]))
    small[0].start()
    for r in range(CHUNKS):
        token_load(r).start()
    small[1].start()
    small[2].start()

    barrier = pltpu.get_barrier_semaphore()
    for other in (partner, across):
        pl.semaphore_signal(barrier, inc=1, device_id={"tp": other}, device_id_type=MESH)
    for other in (next_y, next_z):
        pl.semaphore_signal(barrier, inc=1, device_id={"seq": other}, device_id_type=MESH)
    greeted = 4
    for step in range(1, steps):
        far = 2 ** step
        for reached, other in ((me + far < blocks, me + far), (me >= far, me - far)):
            greeted = greeted + reached.astype(jnp.int32)

            @pl.when(reached)
            def _():
                pl.semaphore_signal(barrier, inc=1, device_id={"seq": other}, device_id_type=MESH)

    quarter = inner // 4
    sub = quarter // SUB

    def strip(owner, j):
        return pl.ds(pl.multiple_of(owner * quarter + j * sub, sub), sub)

    def on_seq(src, dst, ssem, rsem, other):
        return pltpu.make_async_remote_copy(
            src, dst, ssem, rsem, device_id={"seq": other}, device_id_type=MESH)

    def to(src, dst, ssem, rsem, other):
        return pltpu.make_async_remote_copy(
            src, dst, ssem, rsem, device_id={"tp": other}, device_id_type=MESH)

    far_wo = wo.at[1 - side]
    place_y = place + 1 - 2 * bit_y
    place_z = place + 2 - 4 * bit_z

    def wx(j):
        return to(ow_hbm.at[strip(place, j)], wo.at[side, strip(place, j)], wxs.at[j], wxr.at[j], across)

    def wy(j):
        at = strip(place, j)
        return on_seq(far_wo.at[at], far_wo.at[at], wys.at[j], wyr.at[j], next_y)

    def wz(j):
        at = strip(place, j)
        return on_seq(far_wo.at[at], far_wo.at[at], wzs.at[j], wzr.at[j], next_z)

    def wc(j):
        at = strip(3 - place, j)
        return to(ow_hbm.at[at], wo.at[side, at], wcs.at[j], wcr.at[j], across)

    def corner(j):
        if j in VIA_Z:
            at = strip(place_y, j)
            return on_seq(far_wo.at[at], far_wo.at[at], wcs.at[j], wcr.at[j], next_z)
        at = strip(place_z, j)
        return on_seq(far_wo.at[at], far_wo.at[at], wcs.at[j], wcr.at[j], next_y)

    far_half = me >= blocks // 2

    def pass_pieces(cond, pieces):
        @pl.when(cond)
        def _():
            for name, j in pieces:
                if "w" in name:
                    wx(j).wait_recv()
                if "y" in name:
                    wy(j).start()
                if "z" in name:
                    wz(j).start()

    near = jnp.logical_not(far_half)

    def pass_corner(j):
        if j in VIA_Z:
            wy(j).wait_recv()
        else:
            wz(j).wait_recv()
        corner(j).start()

    runs = rows // 128
    tri = (
        lax.broadcasted_iota(jnp.int32, (128, 128), 0)
        <= lax.broadcasted_iota(jnp.int32, (128, 128), 1)
    ).astype(F32).astype(BF16)
    small[0].wait()
    rounded = []
    for b in range(runs):
        left = fgt[:, 128 * b : 128 * b + 128]
        for _ in range(3):
            top = left.astype(BF16).astype(F32)
            rounded.append(top)
            left = left - top
    sums = dot(jnp.concatenate(rounded, axis=0).astype(BF16), tri)
    carried = jnp.zeros((heads, 1), F32)
    for b in range(runs):
        at = 3 * heads * b
        run = sums[at : at + heads] + sums[at + heads : at + 2 * heads]
        run = run + sums[at + 2 * heads : at + 3 * heads] + carried
        ldt[:, 128 * b : 128 * b + 128] = run
        ld[128 * b : 128 * b + 128, :] = run.T
        carried = run[:, 127:128]
    loads[0].start()

    def enter():
        pl.semaphore_wait(barrier, greeted)
        for j in range(SUB):
            wx(j).start()
        for j in STRAIGHT:
            wc(j).start()

    pl.when(me >= blocks // 2)(enter)

    def norm_chunk(r, carry):
        at = pl.ds(pl.multiple_of(r * chunk, chunk), chunk)
        token_load(r).wait()
        normed[at, :] = normalize(tok[at, :].astype(F32), again[...])
        return carry

    loads[1].start()
    small[1].wait()
    small[2].wait()
    lax.fori_loop(0, CHUNKS, norm_chunk, 0)

    def project(weight, dst):
        tile = min(256, dst.shape[1])

        def body(j, carry):
            at = pl.ds(pl.multiple_of(j * tile, tile), tile)
            dst[:, at] = dot(normed[...], weight[:, at]).astype(BF16)
            return carry

        lax.fori_loop(0, dst.shape[1] // tile, body, 0)

    loads[2].start()
    loads[3].start()
    loads[0].wait()
    for c in range(2):
        cols = slice(c * (inner // 2), (c + 1) * (inner // 2))
        k[:, cols] = dot(normed[...], wk[:, cols]).astype(BF16)
    pl.when(near)(enter)
    loads[1].wait()

    low = lax.broadcasted_iota(jnp.int32, (1, 128), 1) < 64
    low_f = low.astype(F32)
    masks_f = (low_f, 1.0 - low_f)
    masks = (masks_f[0].astype(BF16), masks_f[1].astype(BF16))

    def spread(columns, p):
        return jnp.where(low, columns[:, 2 * p : 2 * p + 1], columns[:, 2 * p + 1 : 2 * p + 2])

    log_decay = ld[...]
    last = log_decay[rows - 1 : rows, :]
    shrink = jnp.exp(ldt[:, rows - 1 : rows] - ldt[...])
    tl[...] = jnp.zeros_like(tl)
    el[...] = jnp.zeros_like(el)
    es[...] = jnp.zeros_like(es)
    for p in range(pairs):
        tl[p : p + 1, :] = spread(last, p)
    part_pairs = pairs // 2

    later = bit_y == 1

    def heir(step):
        return me + 2 ** step if step else next_y

    def sends(step):
        return me + 2 ** step < blocks if step else me >= 0

    def takes(step):
        return me >= 2 ** step if step else me >= 0

    def state_copy(step, part_of):
        at = slice(64 * part_pairs * part_of, 64 * part_pairs * (part_of + 1))
        return pltpu.make_async_remote_copy(
            tsb.at[step, at], trb.at[step, at], sts.at[step, part_of], strv.at[step, part_of],
            device_id={"seq": heir(step)}, device_id_type=MESH)

    def decay_copy(step):
        return pltpu.make_async_remote_copy(
            tsl.at[step], trl.at[step], sts.at[step, 2], strv.at[step, 2],
            device_id={"seq": heir(step)}, device_id_type=MESH)

    def state_copies(step):
        return (decay_copy(step), state_copy(step, 0), state_copy(step, 1))

    def send_state(step, part_of):
        @pl.when(sends(step))
        def _():
            at = slice(64 * part_pairs * part_of, 64 * part_pairs * (part_of + 1))
            if part_of == 0:
                tsl[step] = tl[...]
                decay_copy(step).start()
            tsb[step, at, :] = ts[at, :].astype(BF16)
            state_copy(step, part_of).start()

    def take_state(step):
        for part_of in range(2):
            @pl.when(takes(step))
            def _():
                if part_of == 0:
                    decay_copy(step).wait_recv()
                    ed[...] = jnp.exp(el[...])
                    td[...] = jnp.exp(tl[...])
                    if step == 0:
                        td[...] = jnp.where(later, td[...], jnp.exp(trl[step]))
                        el[...] = jnp.where(later, trl[step], el[...])
                    else:
                        el[...] = el[...] + trl[step]
                    tl[...] = tl[...] + trl[step]
                state_copy(step, part_of).wait_recv()
                for p in range(part_pairs * part_of, part_pairs * (part_of + 1)):
                    at = slice(64 * p, 64 * p + 64)
                    came = trb[step, at, :].astype(F32)
                    decay = td[p : p + 1, :]
                    if step == 0:
                        mine_first = ts[at, :]
                        es[at, :] = jnp.where(later, came, 0.0)
                        ts[at, :] = jnp.where(
                            later, mine_first + decay * came, decay * mine_first + came)
                    else:
                        es[at, :] = es[at, :] + ed[p : p + 1, :] * came
                        ts[at, :] = ts[at, :] + decay * came

            if step + 1 < steps:
                send_state(step + 1, part_of)

    for p in range(pairs):
        turned = k[:, 128 * p : 128 * p + 128].T.astype(F32)
        for j in range(2):
            h = 2 * p + j
            ks[64 * h : 64 * h + 64, :] = (turned[64 * j : 64 * j + 64] * shrink[h : h + 1, :]).astype(BF16)
    each = 128 * part_pairs
    for part_of in range(2):
        cols = slice(each * part_of, each * (part_of + 1))
        v[:, cols] = dot(normed[...], wv[:, cols]).astype(BF16)
        state = dot(ks[cols, :], v[:, cols])
        for p in range(part_pairs):
            at = slice(128 * p, 128 * p + 128)
            pair = state[at, at]
            h = 64 * (part_pairs * part_of + p)
            ts[h : h + 64, :] = pair[:64] * masks_f[0] + pair[64:] * masks_f[1]
        send_state(0, part_of)

    for at in (4, 5, 6):
        loads[at].start()
    loads[2].wait()
    pass_pieces(far_half, (("wz", 0), ("wz", 1)))
    project(wq, q)

    span = rows // 2
    taken = 0
    for p in range(pairs):
        lanes = slice(128 * p, 128 * p + 128)
        for piece in range(2):
            at = slice(piece * span, piece * span + span)
            reach = (piece + 1) * span
            causal = (
                lax.broadcasted_iota(jnp.int32, (span, reach), 0) + piece * span
                >= lax.broadcasted_iota(jnp.int32, (span, reach), 1)
            )
            sums = []
            for j in range(2):
                h = 2 * p + j
                scores = contract(q[at, lanes] * masks[j], k[:reach, lanes], 1, 1)
                gaps = jnp.where(causal, ld[at, h : h + 1] - ldt[h : h + 1, :reach], -1e30)
                weights = (scores * 0.125 * jnp.exp(gaps)).astype(BF16)
                sums.append(dot(weights, v[:reach, lanes]))
            att[at, lanes] = jnp.where(low, sums[0], sums[1])
            if p % 2 == 0 and piece and taken < steps:
                take_state(taken)
                taken += 1
                if taken == 1:
                    pass_pieces(far_half, (("y", 0), ("y", 1), ("wy", 2)))
                elif taken == 2:
                    pass_pieces(far_half, (("wy", 4),))
                    pass_pieces(near, (("wyz", 0),))
        if p == 1:
            pass_pieces(far_half, (("wy", 3),))
        if p == pairs - 1:
            pass_pieces(far_half, (("wy", 5),))
            pass_pieces(near, (("wyz", 1),))
    while taken < steps:
        take_state(taken)
        taken += 1

    pass_pieces(far_half, [("z", j) for j in range(2, 6)] + [("wyz", 6)])

    for p in range(pairs):
        came = es[64 * p : 64 * p + 64, :]
        bd[p] = jnp.concatenate([came * masks_f[0], came * masks_f[1]], axis=0).astype(BF16)
    same_head = (
        (lax.broadcasted_iota(jnp.int32, (128, 128), 0) < 64)
        == (lax.broadcasted_iota(jnp.int32, (128, 128), 1) < 64)
    ).astype(F32).astype(BF16)

    starts, total = [], 0
    for size in SIZES:
        starts.append(total * (rows // sum(SIZES)))
        total += size
    sizes = [size * (rows // sum(SIZES)) for size in SIZES]
    count = len(sizes)

    def whole_rows(r):
        return slice(starts[r], starts[r] + sizes[r])

    def half_rows(r):
        return slice(starts[r] // 2, starts[r] // 2 + sizes[r] // 2)

    def own_rows(r):
        half = sizes[r] // 2
        return pl.ds(pl.multiple_of(starts[r] + core * half, half), half)

    def mine(r):
        half = sizes[r] // 2
        return pl.ds(pl.multiple_of(core * half, half), half)

    def theirs(r):
        half = sizes[r] // 2
        return pl.ds(pl.multiple_of(half - core * half, half), half)

    def d1(r):
        at = half_rows(r)
        return to(dsend1.at[at], drecv1.at[at], d1s.at[r], d1r.at[r], partner)

    def x1(r):
        at = half_rows(r)
        return to(xsend1.at[at], xrecv1.at[at], x1s.at[r], x1r.at[r], across)

    def hx(r):
        at = whole_rows(r)
        return to(ho.at[side, at], ho.at[side, at], hs.at[r], hr.at[r], across)

    def nfc(r):
        return to(nf.at[own_rows(r)], nf.at[own_rows(r)], ns.at[r], nr.at[r], partner)

    def d2(r):
        at = half_rows(r)
        return to(dsend2.at[at], drecv2.at[at], d2s.at[r], d2r.at[r], partner)

    def x2(r, piece):
        n = sizes[r] // 4
        at = pl.ds(starts[r] // 2 + piece * n, n)
        return to(xsend2.at[at], xrecv2.at[at], x2s.at[r, piece], x2r.at[r, piece], across)

    def oc(r, piece):
        at = out_rows(r, piece)
        return to(out.at[at], out.at[at], osd.at[r, piece], orv.at[r, piece], partner)

    def out_rows(r, piece):
        n = sizes[r] // 4
        return pl.ds(pl.multiple_of(starts[r] + core * 2 * n + piece * n, n), n)

    loads[3].wait()
    wide = min(512, width)

    def attend(r):
        at = whole_rows(r)
        reach_decay = jnp.exp(ld[at, :]) * 0.125
        for p in range(pairs):
            lanes = slice(128 * p, 128 * p + 128)
            attended = att[at, lanes] + dot(q[at, lanes], bd[p]) * spread(reach_decay, p)
            mean_square = dot((attended * attended).astype(BF16), same_head) * (1.0 / 64)
            ho[side, at, lanes] = (attended * lax.rsqrt(mean_square + head_epsilon)).astype(BF16)

    def halve(r, send, copy):
        n = sizes[r]
        own[half_rows(r), :] = part[mine(r), :]
        send[half_rows(r), :] = part[theirs(r), :].astype(BF16)
        copy.start()

    def combine(r):
        at, n = whole_rows(r), sizes[r]
        for c in range(width // wide):
            cols = slice(c * wide, c * wide + wide)
            if r < PLAIN:
                part[:n, cols] = dot(ho[side, at, :], wo[side, :, cols])
            else:
                part[:n, cols] = dot(ho[0, at, :], wo[0, :, cols]) + dot(ho[1, at, :], wo[1, :, cols])
        halve(r, dsend1, d1(r))

    def cross(r):
        at = half_rows(r)
        d1(r).wait_recv()
        xsend1[at, :] = (own[at, :] + drecv1[at, :].astype(F32)).astype(BF16)
        x1(r).start()

    def settle(r):
        at = half_rows(r)
        if r < PLAIN:
            x1(r).wait_recv()
            added = xsend1[at, :].astype(F32) + xrecv1[at, :].astype(F32)
        else:
            d1(r).wait_recv()
            added = own[at, :] + drecv1[at, :].astype(F32)
        kept = (tok[own_rows(r), :].astype(F32) + added).astype(BF16)
        res[at, :] = kept
        nf[own_rows(r), :] = normalize(kept.astype(F32), fgain[...])
        nfc(r).start()

    hidden_width = wg.shape[1]
    tile = min(256, hidden_width)

    def forward(r):
        nfc(r).wait_recv()
        at, n = whole_rows(r), sizes[r]
        for c in range(hidden_width // tile):
            cols = slice(c * tile, c * tile + tile)
            gate = dot(nf[at, :], wg[:, cols])
            up = dot(nf[at, :], wu[:, cols])
            hid[:n, cols] = (gate / (1.0 + jnp.exp(-gate)) * up).astype(BF16)
        for c in range(width // wide):
            cols = slice(c * wide, c * wide + wide)
            part[:n, cols] = dot(hid[:n, :], wd[:, cols])
        halve(r, dsend2, d2(r))

    def pass_sums(r):
        at = half_rows(r)
        d2(r).wait_recv()
        xsend2[at, :] = (own[at, :] + drecv2[at, :].astype(F32)).astype(BF16)
        x2(r, 0).start()
        x2(r, 1).start()

    def finish(r, piece):
        n = sizes[r] // 4
        at = slice(starts[r] // 2 + piece * n, starts[r] // 2 + piece * n + n)
        x2(r, piece).wait_recv()
        added = xsend2[at, :].astype(F32) + xrecv2[at, :].astype(F32)
        out[out_rows(r, piece), :] = (res[at, :].astype(F32) + added).astype(BF16)
        oc(r, piece).start()

    if PLAIN < count:
        attend(PLAIN)
        hx(PLAIN).start()
    for r in range(PLAIN):
        attend(r)
        combine(r)
    pass_pieces(far_half, (("wyz", 7),))
    pass_pieces(near, (("wyz", 2), ("wyz", 3)))
    for r in range(PLAIN + 1, count):
        attend(r)
    for r in range(PLAIN):
        cross(r)
    for r in range(PLAIN + 1, count):
        hx(r).start()
    pass_pieces(near, [("wyz", j) for j in range(4, SUB)])
    for at in (4, 5, 6):
        loads[at].wait()

    def arrive():
        for j in range(SUB):
            if j not in VIA_Z:
                wy(j).wait_recv()
            if j not in VIA_Y:
                wz(j).wait_recv()
            if j in STRAIGHT:
                wc(j).wait_recv()
            else:
                corner(j).wait_recv()

    def combine_late(r):
        if r == PLAIN:
            arrive()
        hx(r).wait_recv()
        combine(r)

    for j in VIA_Z + VIA_Y:
        pass_corner(j)
    settle(0)
    for r in range(count):
        if PLAIN < r + 1 < count:
            combine_late(r + 1)
        if r > PLAIN:
            pass_sums(r - 1)
        forward(r)
        if r + 1 == PLAIN < count:
            combine_late(r + 1)
        if r < PLAIN:
            pass_sums(r)
        if r + 1 < count:
            settle(r + 1)
    pass_sums(count - 1)
    for j in range(SUB):
        for copy in (wx(j), wy(j), wz(j), wc(j) if j in STRAIGHT else corner(j)):
            copy.wait_send()
    for step in range(steps):
        @pl.when(sends(step))
        def _():
            for copy in state_copies(step):
                copy.wait_send()
    for r in range(count):
        for copy in (d1(r), nfc(r), d2(r), x1(r) if r < PLAIN else hx(r)):
            copy.wait_send()
    for r in range(count):
        for piece in range(2):
            finish(r, piece)
    for r in range(count):
        for piece in range(2):
            x2(r, piece).wait_send()
            oc(r, piece).wait()


def local(blocks, tokens, forget, attn_gain, projections, out_weight, ffn_gain, expand_weight, down_weight):
    rows, width = tokens.shape
    heads = forget.shape[1]
    inner = projections.shape[2]
    hidden = down_weight.shape[0]
    pairs = heads // 2
    steps = max(blocks - 1, 0).bit_length()
    V = pltpu.VMEM
    S = pltpu.SemaphoreType.DMA
    slots = max(steps, 1)
    count = len(SIZES)
    largest = rows // sum(SIZES) * max(SIZES)
    halves = V((rows // 2, width), BF16)
    early = V((rows // sum(SIZES) * sum(SIZES[:max(PLAIN, 1)]) // 2, width), BF16)
    scratch = [
        V((heads, rows), F32), V((1, width), F32), V((1, width), F32),
        V((rows, width), BF16),
        V((width, inner), BF16), V((width, inner), BF16), V((width, inner), BF16),
        V((2, inner, width), BF16),
        V((width, hidden), BF16), V((width, hidden), BF16), V((hidden, width), BF16),
        V((rows, width), BF16),
        V((rows, inner), BF16), V((rows, inner), BF16), V((rows, inner), BF16),
        V((rows, inner), F32), V((2, rows, inner), BF16),
        V((pairs, 128, 128), BF16),
        V((64 * pairs, 128), F32), V((8, 128), F32), V((64 * pairs, 128), F32), V((8, 128), F32),
        V((8, 128), F32), V((8, 128), F32),
        V((slots, 64 * pairs, 128), BF16), V((slots, 8, 128), F32),
        V((slots, 64 * pairs, 128), BF16), V((slots, 8, 128), F32),
        V((largest, width), F32), V((rows // 2, width), F32),
        halves, halves, early, early,
        V((rows, width), BF16), halves, V((largest, hidden), BF16),
        halves, halves, halves, halves,
        V((inner, rows), BF16), V((rows, heads), F32), V((heads, rows), F32),
        S((8,)), S((CHUNKS,)), S((3,)), S((slots, 3)), S((slots, 3)),
    ] + [S((SUB,)) for _ in range(8)] + [S((count,)) for _ in range(10)] + [S((count, 2)) for _ in range(4)]
    hbm = pl.BlockSpec(memory_space=pl.ANY)
    vmem = pl.BlockSpec(memory_space=pltpu.VMEM)
    return pl.pallas_call(
        functools.partial(kernel, blocks, steps),
        out_shape=pltpu.VMEM((rows, width), BF16),
        in_specs=[hbm] * 8,
        out_specs=vmem,
        scratch_shapes=scratch,
        compiler_params=pltpu.CompilerParams(
            collective_id=0, has_side_effects=True, vmem_limit_bytes=60_000_000
        ),
    )(
        tokens, forget.T, attn_gain[None, :], projections, out_weight,
        ffn_gain[None, :], expand_weight, down_weight,
    )


def solution(mesh):
    placed = (
        P("seq", None),
        P("seq", "tp"),
        P(),
        P(None, None, "tp"),
        P("tp", None),
        P(),
        P(None, None, "tp"),
        P("tp", None),
    )
    return jax.shard_map(
        functools.partial(local, mesh.shape["seq"]),
        mesh=mesh, in_specs=placed, out_specs=P("seq", None), check_vma=False,
    )
```

```python
import functools

import jax
import jax.numpy as jnp
from jax import lax
from jax.experimental import pallas as pl
from jax.experimental.pallas import tpu as pltpu
from jax.sharding import PartitionSpec as P

norm_epsilon = 1e-05
head_epsilon = 1e-06
MESH = pl.DeviceIdType.MESH
CHUNKS = 4
SIZES = (2, 2, 2, 2)
PLAIN = 1
SUB = 8
FAR_Z = (0,)
FAR_X = (6, 7)
NEAR_Z = (0, 1, 2, 3)
NEAR_X = ()
F32 = jnp.float32
BF16 = jnp.bfloat16


def dot(a, b):
    return jnp.dot(a, b, preferred_element_type=F32)


def contract(a, b, dim_a, dim_b):
    return lax.dot_general(
        a, b, (((dim_a,), (dim_b,)), ((), ())), preferred_element_type=F32
    )


def normalize(widened, gain):
    mean_square = jnp.mean(widened * widened, axis=-1, keepdims=True)
    return (widened * lax.rsqrt(mean_square + norm_epsilon) * gain).astype(BF16)


def kernel(
    blocks, steps,
    tok_hbm, fgt_hbm, again_hbm, proj_hbm, ow_hbm, fgain_hbm, ew_hbm, dw_hbm,
    out,
    fgt, again, fgain,
    tok, wq, wk, wv, wo, wg, wu, wd,
    normed, q, k, v, att, ho, bd, es, el, ts, tl, ed, td, tsb, tsl, trb, trl,
    part, own, dsend1, drecv1, xsend1, xrecv1, nf, res, hid,
    dsend2, drecv2, xsend2, xrecv2,
    ks, ld, ldt,
    wsem, tsem, small_sem, sts, strv, wxs, wxr, wys, wyr, wzs, wzr, wcs, wcr,
    d1s, d1r, x1s, x1r, hs, hr, ns, nr, d2s, d2r, x2s, x2r, osd, orv,
):
    rows, width = tok.shape
    heads = fgt.shape[0]
    inner = wk.shape[1]
    pairs = heads // 2
    chunk = rows // CHUNKS
    me = lax.axis_index("seq")
    tp = lax.axis_index("tp")
    core = lax.rem(tp, 2)
    side = lax.div(tp, 2)
    partner = tp + 1 - 2 * core
    across = lax.rem(tp + 2, 4)
    place = lax.rem(me, 4)
    bit_y = lax.rem(me, 2)
    bit_z = lax.div(place, 2)
    next_y = me + 1 - 2 * bit_y
    next_z = me + 2 - 4 * bit_z

    loads = []
    for at, (src, dst) in enumerate((
        (proj_hbm.at[1], wk), (proj_hbm.at[2], wv), (proj_hbm.at[0], wq),
        (ow_hbm, wo.at[side]), (ew_hbm.at[0], wg), (ew_hbm.at[1], wu), (dw_hbm, wd),
    )):
        copy = pltpu.make_async_copy(src, dst, wsem.at[at])
        loads.append(copy)
    def token_load(r):
        at = pl.ds(pl.multiple_of(r * chunk, chunk), chunk)
        return pltpu.make_async_copy(tok_hbm.at[at], tok.at[at], tsem.at[r])

    small = []
    for at, (src, dst) in enumerate(((fgt_hbm, fgt), (again_hbm, again), (fgain_hbm, fgain))):
        small.append(pltpu.make_async_copy(src, dst, small_sem.at[at]))
    small[0].start()
    for r in range(CHUNKS):
        token_load(r).start()
    small[1].start()
    small[2].start()

    barrier = pltpu.get_barrier_semaphore()
    for other in (partner, across):
        pl.semaphore_signal(barrier, inc=1, device_id={"tp": other}, device_id_type=MESH)
    for other in (next_y, next_z):
        pl.semaphore_signal(barrier, inc=1, device_id={"seq": other}, device_id_type=MESH)
    greeted = 4
    for step in range(1, steps):
        far = 2 ** step
        for reached, other in ((me + far < blocks, me + far), (me >= far, me - far)):
            greeted = greeted + reached.astype(jnp.int32)

            @pl.when(reached)
            def _():
                pl.semaphore_signal(barrier, inc=1, device_id={"seq": other}, device_id_type=MESH)

    quarter = inner // 4
    sub = quarter // SUB

    def strip(owner, j):
        return pl.ds(pl.multiple_of(owner * quarter + j * sub, sub), sub)

    def on_seq(src, dst, ssem, rsem, other):
        return pltpu.make_async_remote_copy(
            src, dst, ssem, rsem, device_id={"seq": other}, device_id_type=MESH)

    def to(src, dst, ssem, rsem, other):
        return pltpu.make_async_remote_copy(
            src, dst, ssem, rsem, device_id={"tp": other}, device_id_type=MESH)

    far_wo = wo.at[1 - side]
    place_y = place + 1 - 2 * bit_y
    place_z = place + 2 - 4 * bit_z

    def wx(j):
        return to(ow_hbm.at[strip(place, j)], wo.at[side, strip(place, j)], wxs.at[0], wxr.at[j], across)

    def wy(j):
        at = strip(place, j)
        return on_seq(far_wo.at[at], far_wo.at[at], wys.at[0], wyr.at[j], next_y)

    def wz(j):
        at = strip(place, j)
        return on_seq(far_wo.at[at], far_wo.at[at], wzs.at[0], wzr.at[j], next_z)

    def wc(j):
        at = strip(3 - place, j)
        return to(ow_hbm.at[at], wo.at[side, at], wcs.at[0], wcr.at[j], across)

    def corner(j, over_z):
        owner, other = (place_y, next_z) if over_z else (place_z, next_y)
        at = strip(owner, j)
        return on_seq(far_wo.at[at], far_wo.at[at], wcs.at[0], wcr.at[j], other)

    far_half = me >= blocks // 2

    def pass_pieces(cond, pieces):
        @pl.when(cond)
        def _():
            for name, j in pieces:
                if "w" in name:
                    wx(j).wait_recv()
                if "y" in name:
                    wy(j).start()
                if "z" in name:
                    wz(j).start()

    near = jnp.logical_not(far_half)

    def by_half(body):
        @pl.when(far_half)
        def _():
            body(FAR_Z, FAR_X)

        @pl.when(near)
        def _():
            body(NEAR_Z, NEAR_X)

    def pass_corners(over_z, straight):
        for j in range(SUB):
            if j in straight:
                continue
            if j in over_z:
                wy(j).wait_recv()
            else:
                wz(j).wait_recv()
            corner(j, j in over_z).start()

    def take_pieces(over_z, straight):
        for j in range(SUB):
            if j in straight or j not in over_z:
                wy(j).wait_recv()
            if j in straight or j in over_z:
                wz(j).wait_recv()
            if j in straight:
                wc(j).wait_recv()
            else:
                corner(j, j in over_z).wait_recv()

    def drain_pieces():
        sent = far_wo.at[pl.ds(pl.multiple_of(place * quarter, quarter), quarter)]
        for sem in (wxs, wys, wzs, wcs):
            to(sent, sent, sem.at[0], wxr.at[0], across).wait_send()

    runs = rows // 128
    tri = (
        lax.broadcasted_iota(jnp.int32, (128, 128), 0)
        <= lax.broadcasted_iota(jnp.int32, (128, 128), 1)
    ).astype(F32).astype(BF16)
    small[0].wait()
    rounded = []
    for b in range(runs):
        left = fgt[:, 128 * b : 128 * b + 128]
        for _ in range(3):
            top = left.astype(BF16).astype(F32)
            rounded.append(top)
            left = left - top
    sums = dot(jnp.concatenate(rounded, axis=0).astype(BF16), tri)
    carried = jnp.zeros((heads, 1), F32)
    for b in range(runs):
        at = 3 * heads * b
        run = sums[at : at + heads] + sums[at + heads : at + 2 * heads]
        run = run + sums[at + 2 * heads : at + 3 * heads] + carried
        ldt[:, 128 * b : 128 * b + 128] = run
        ld[128 * b : 128 * b + 128, :] = run.T
        carried = run[:, 127:128]
    loads[0].start()

    def enter(straight):
        pl.semaphore_wait(barrier, greeted)
        for j in range(SUB):
            wx(j).start()
        for j in straight:
            wc(j).start()

    @pl.when(far_half)
    def _():
        enter(FAR_X)

    def norm_chunk(r, carry):
        at = pl.ds(pl.multiple_of(r * chunk, chunk), chunk)
        token_load(r).wait()
        normed[at, :] = normalize(tok[at, :].astype(F32), again[...])
        return carry

    loads[1].start()
    small[1].wait()
    small[2].wait()
    lax.fori_loop(0, CHUNKS, norm_chunk, 0)

    def project(weight, dst):
        tile = min(256, dst.shape[1])

        def body(j, carry):
            at = pl.ds(pl.multiple_of(j * tile, tile), tile)
            dst[:, at] = dot(normed[...], weight[:, at]).astype(BF16)
            return carry

        lax.fori_loop(0, dst.shape[1] // tile, body, 0)

    loads[2].start()
    loads[3].start()
    loads[0].wait()
    for c in range(2):
        cols = slice(c * (inner // 2), (c + 1) * (inner // 2))
        k[:, cols] = dot(normed[...], wk[:, cols]).astype(BF16)

    @pl.when(near)
    def _():
        enter(NEAR_X)

    loads[1].wait()

    low = lax.broadcasted_iota(jnp.int32, (1, 128), 1) < 64
    low_f = low.astype(F32)
    masks_f = (low_f, 1.0 - low_f)
    masks = (masks_f[0].astype(BF16), masks_f[1].astype(BF16))

    def spread(columns, p):
        return jnp.where(low, columns[:, 2 * p : 2 * p + 1], columns[:, 2 * p + 1 : 2 * p + 2])

    log_decay = ld[...]
    last = log_decay[rows - 1 : rows, :]
    shrink = jnp.exp(ldt[:, rows - 1 : rows] - ldt[...])
    tl[...] = jnp.zeros_like(tl)
    el[...] = jnp.zeros_like(el)
    es[...] = jnp.zeros_like(es)
    for p in range(pairs):
        tl[p : p + 1, :] = spread(last, p)
    part_pairs = pairs // 2

    later = bit_y == 1

    def heir(step):
        return me + 2 ** step if step else next_y

    def sends(step):
        return me + 2 ** step < blocks if step else me >= 0

    def takes(step):
        return me >= 2 ** step if step else me >= 0

    def state_copy(step, part_of):
        at = slice(64 * part_pairs * part_of, 64 * part_pairs * (part_of + 1))
        return pltpu.make_async_remote_copy(
            tsb.at[step, at], trb.at[step, at], sts.at[step, part_of], strv.at[step, part_of],
            device_id={"seq": heir(step)}, device_id_type=MESH)

    def decay_copy(step):
        return pltpu.make_async_remote_copy(
            tsl.at[step], trl.at[step], sts.at[step, 2], strv.at[step, 2],
            device_id={"seq": heir(step)}, device_id_type=MESH)

    def state_copies(step):
        return (decay_copy(step), state_copy(step, 0), state_copy(step, 1))

    def send_state(step, part_of):
        @pl.when(sends(step))
        def _():
            at = slice(64 * part_pairs * part_of, 64 * part_pairs * (part_of + 1))
            if part_of == 0:
                tsl[step] = tl[...]
                decay_copy(step).start()
            tsb[step, at, :] = ts[at, :].astype(BF16)
            state_copy(step, part_of).start()

    def take_state(step):
        for part_of in range(2):
            @pl.when(takes(step))
            def _():
                if part_of == 0:
                    decay_copy(step).wait_recv()
                    ed[...] = jnp.exp(el[...])
                    td[...] = jnp.exp(tl[...])
                    if step == 0:
                        td[...] = jnp.where(later, td[...], jnp.exp(trl[step]))
                        el[...] = jnp.where(later, trl[step], el[...])
                    else:
                        el[...] = el[...] + trl[step]
                    tl[...] = tl[...] + trl[step]
                state_copy(step, part_of).wait_recv()
                for p in range(part_pairs * part_of, part_pairs * (part_of + 1)):
                    at = slice(64 * p, 64 * p + 64)
                    came = trb[step, at, :].astype(F32)
                    decay = td[p : p + 1, :]
                    if step == 0:
                        mine_first = ts[at, :]
                        es[at, :] = jnp.where(later, came, 0.0)
                        ts[at, :] = jnp.where(
                            later, mine_first + decay * came, decay * mine_first + came)
                    else:
                        es[at, :] = es[at, :] + ed[p : p + 1, :] * came
                        ts[at, :] = ts[at, :] + decay * came

            if step + 1 < steps:
                send_state(step + 1, part_of)

    for p in range(pairs):
        turned = k[:, 128 * p : 128 * p + 128].T.astype(F32)
        for j in range(2):
            h = 2 * p + j
            ks[64 * h : 64 * h + 64, :] = (turned[64 * j : 64 * j + 64] * shrink[h : h + 1, :]).astype(BF16)
    each = 128 * part_pairs
    for part_of in range(2):
        cols = slice(each * part_of, each * (part_of + 1))
        v[:, cols] = dot(normed[...], wv[:, cols]).astype(BF16)
        state = dot(ks[cols, :], v[:, cols])
        for p in range(part_pairs):
            at = slice(128 * p, 128 * p + 128)
            pair = state[at, at]
            h = 64 * (part_pairs * part_of + p)
            ts[h : h + 64, :] = pair[:64] * masks_f[0] + pair[64:] * masks_f[1]
        send_state(0, part_of)

    for at in (4, 5, 6):
        loads[at].start()
    loads[2].wait()
    pass_pieces(far_half, (("wz", 0), ("wz", 1)))
    project(wq, q)

    span = rows // 2
    taken = 0
    for p in range(pairs):
        lanes = slice(128 * p, 128 * p + 128)
        for piece in range(2):
            at = slice(piece * span, piece * span + span)
            reach = (piece + 1) * span
            causal = (
                lax.broadcasted_iota(jnp.int32, (span, reach), 0) + piece * span
                >= lax.broadcasted_iota(jnp.int32, (span, reach), 1)
            )
            sums = []
            for j in range(2):
                h = 2 * p + j
                scores = contract(q[at, lanes] * masks[j], k[:reach, lanes], 1, 1)
                gaps = jnp.where(causal, ld[at, h : h + 1] - ldt[h : h + 1, :reach], -1e30)
                weights = (scores * 0.125 * jnp.exp(gaps)).astype(BF16)
                sums.append(dot(weights, v[:reach, lanes]))
            att[at, lanes] = jnp.where(low, sums[0], sums[1])
            if p == 0 and piece:
                pass_pieces(near, (("wy", 0), ("wy", 1)))
            if p % 2 == 0 and piece and taken < steps:
                take_state(taken)
                taken += 1
                if taken == 1:
                    pass_pieces(far_half, (("y", 0), ("y", 1), ("wy", 2)))
                elif taken == 2:
                    pass_pieces(far_half, (("wy", 4),))
                    pass_pieces(near, (("z", 0), ("z", 1), ("z", 2), ("wyz", 3)))
        if p == 1:
            pass_pieces(far_half, (("wy", 3),))
            pass_pieces(near, (("wy", 2),))
        if p == pairs - 1:
            pass_pieces(far_half, (("wy", 5),))
            pass_pieces(near, (("wyz", 4),))
    while taken < steps:
        take_state(taken)
        taken += 1

    pass_pieces(far_half, [("z", j) for j in range(2, 6)] + [("wyz", 6)])

    for p in range(pairs):
        came = es[64 * p : 64 * p + 64, :]
        bd[p] = jnp.concatenate([came * masks_f[0], came * masks_f[1]], axis=0).astype(BF16)
    same_head = (
        (lax.broadcasted_iota(jnp.int32, (128, 128), 0) < 64)
        == (lax.broadcasted_iota(jnp.int32, (128, 128), 1) < 64)
    ).astype(F32).astype(BF16)

    starts, total = [], 0
    for size in SIZES:
        starts.append(total * (rows // sum(SIZES)))
        total += size
    sizes = [size * (rows // sum(SIZES)) for size in SIZES]
    count = len(sizes)

    def whole_rows(r):
        return slice(starts[r], starts[r] + sizes[r])

    def half_rows(r):
        return slice(starts[r] // 2, starts[r] // 2 + sizes[r] // 2)

    def own_rows(r):
        half = sizes[r] // 2
        return pl.ds(pl.multiple_of(starts[r] + core * half, half), half)

    def mine(r):
        half = sizes[r] // 2
        return pl.ds(pl.multiple_of(core * half, half), half)

    def theirs(r):
        half = sizes[r] // 2
        return pl.ds(pl.multiple_of(half - core * half, half), half)

    def d1(r):
        at = half_rows(r)
        return to(dsend1.at[at], drecv1.at[at], d1s.at[0], d1r.at[r], partner)

    def x1(r):
        at = half_rows(r)
        return to(xsend1.at[at], xrecv1.at[at], x1s.at[0], x1r.at[r], across)

    def hx(r):
        at = whole_rows(r)
        return to(ho.at[side, at], ho.at[side, at], hs.at[0], hr.at[r], across)

    def nfc(r):
        return to(nf.at[own_rows(r)], nf.at[own_rows(r)], ns.at[0], nr.at[r], partner)

    def d2(r):
        at = half_rows(r)
        return to(dsend2.at[at], drecv2.at[at], d2s.at[0], d2r.at[r], partner)

    def x2(r, piece):
        n = sizes[r] // 4
        at = pl.ds(starts[r] // 2 + piece * n, n)
        return to(xsend2.at[at], xrecv2.at[at], x2s.at[0], x2r.at[r, piece], across)

    def oc(r, piece):
        at = out_rows(r, piece)
        return to(out.at[at], out.at[at], osd.at[0], orv.at[0], partner)

    def out_rows(r, piece):
        n = sizes[r] // 4
        return pl.ds(pl.multiple_of(starts[r] + core * 2 * n + piece * n, n), n)

    loads[3].wait()
    wide = min(512, width)

    def attend(r):
        at = whole_rows(r)
        reach_decay = jnp.exp(ld[at, :]) * 0.125
        for p in range(pairs):
            lanes = slice(128 * p, 128 * p + 128)
            attended = att[at, lanes] + dot(q[at, lanes], bd[p]) * spread(reach_decay, p)
            mean_square = dot((attended * attended).astype(BF16), same_head) * (1.0 / 64)
            ho[side, at, lanes] = (attended * lax.rsqrt(mean_square + head_epsilon)).astype(BF16)

    def halve(r, send, copy):
        n = sizes[r]
        own[half_rows(r), :] = part[mine(r), :]
        send[half_rows(r), :] = part[theirs(r), :].astype(BF16)
        copy.start()

    def combine(r):
        at, n = whole_rows(r), sizes[r]
        for c in range(width // wide):
            cols = slice(c * wide, c * wide + wide)
            if r < PLAIN:
                part[:n, cols] = dot(ho[side, at, :], wo[side, :, cols])
            else:
                part[:n, cols] = dot(ho[0, at, :], wo[0, :, cols]) + dot(ho[1, at, :], wo[1, :, cols])
        halve(r, dsend1, d1(r))

    def cross(r):
        at = half_rows(r)
        d1(r).wait_recv()
        xsend1[at, :] = (own[at, :] + drecv1[at, :].astype(F32)).astype(BF16)
        x1(r).start()

    def settle(r):
        at = half_rows(r)
        if r < PLAIN:
            x1(r).wait_recv()
            added = xsend1[at, :].astype(F32) + xrecv1[at, :].astype(F32)
        else:
            d1(r).wait_recv()
            added = own[at, :] + drecv1[at, :].astype(F32)
        kept = (tok[own_rows(r), :].astype(F32) + added).astype(BF16)
        res[at, :] = kept
        nf[own_rows(r), :] = normalize(kept.astype(F32), fgain[...])
        nfc(r).start()

    hidden_width = wg.shape[1]
    tile = min(256, hidden_width)

    def forward(r):
        nfc(r).wait_recv()
        at, n = whole_rows(r), sizes[r]
        for c in range(hidden_width // tile):
            cols = slice(c * tile, c * tile + tile)
            gate = dot(nf[at, :], wg[:, cols])
            up = dot(nf[at, :], wu[:, cols])
            hid[:n, cols] = (gate / (1.0 + jnp.exp(-gate)) * up).astype(BF16)
        for c in range(width // wide):
            cols = slice(c * wide, c * wide + wide)
            part[:n, cols] = dot(hid[:n, :], wd[:, cols])
        halve(r, dsend2, d2(r))

    def pass_sums(r):
        at = half_rows(r)
        d2(r).wait_recv()
        xsend2[at, :] = (own[at, :] + drecv2[at, :].astype(F32)).astype(BF16)
        x2(r, 0).start()
        x2(r, 1).start()

    def finish(r, piece):
        n = sizes[r] // 4
        at = slice(starts[r] // 2 + piece * n, starts[r] // 2 + piece * n + n)
        x2(r, piece).wait_recv()
        added = xsend2[at, :].astype(F32) + xrecv2[at, :].astype(F32)
        out[out_rows(r, piece), :] = (res[at, :].astype(F32) + added).astype(BF16)
        oc(r, piece).start()

    if PLAIN < count:
        attend(PLAIN)
        hx(PLAIN).start()
    for r in range(PLAIN):
        attend(r)
        combine(r)
    pass_pieces(far_half, (("wyz", 7),))
    pass_pieces(near, (("wyz", 5),))
    for r in range(PLAIN + 1, count):
        attend(r)
    for r in range(PLAIN):
        cross(r)
    for r in range(PLAIN + 1, count):
        hx(r).start()
    pass_pieces(near, [("wyz", j) for j in range(6, SUB)])
    for at in (4, 5, 6):
        loads[at].wait()

    def arrive():
        by_half(take_pieces)

    def combine_late(r):
        if r == PLAIN:
            arrive()
        hx(r).wait_recv()
        combine(r)

    by_half(pass_corners)
    settle(0)
    for r in range(count):
        if PLAIN < r + 1 < count:
            combine_late(r + 1)
        if r > PLAIN:
            pass_sums(r - 1)
        forward(r)
        if r + 1 == PLAIN < count:
            combine_late(r + 1)
        if r < PLAIN:
            pass_sums(r)
        if r + 1 < count:
            settle(r + 1)
    pass_sums(count - 1)
    drain_pieces()
    for step in range(steps):
        @pl.when(sends(step))
        def _():
            for copy in state_copies(step):
                copy.wait_send()
    to(dsend1, dsend1, d1s.at[0], d1r.at[0], partner).wait_send()
    to(dsend1, dsend1, ns.at[0], nr.at[0], partner).wait_send()
    to(dsend2, dsend2, d2s.at[0], d2r.at[0], partner).wait_send()
    if PLAIN:
        to(xsend1, xsend1, x1s.at[0], x1r.at[0], across).wait_send()
    if PLAIN < count:
        late = ho.at[side, slice(starts[PLAIN], rows)]
        to(late, late, hs.at[0], hr.at[PLAIN], across).wait_send()
    for r in range(count):
        for piece in range(2):
            finish(r, piece)
    to(xsend2, xsend2, x2s.at[0], x2r.at[0, 0], across).wait_send()
    to(xsend2, xrecv2, osd.at[0], orv.at[0], partner).wait()


def local(blocks, tokens, forget, attn_gain, projections, out_weight, ffn_gain, expand_weight, down_weight):
    rows, width = tokens.shape
    heads = forget.shape[1]
    inner = projections.shape[2]
    hidden = down_weight.shape[0]
    pairs = heads // 2
    steps = max(blocks - 1, 0).bit_length()
    V = pltpu.VMEM
    S = pltpu.SemaphoreType.DMA
    slots = max(steps, 1)
    count = len(SIZES)
    largest = rows // sum(SIZES) * max(SIZES)
    halves = V((rows // 2, width), BF16)
    early = V((rows // sum(SIZES) * sum(SIZES[:max(PLAIN, 1)]) // 2, width), BF16)
    scratch = [
        V((heads, rows), F32), V((1, width), F32), V((1, width), F32),
        V((rows, width), BF16),
        V((width, inner), BF16), V((width, inner), BF16), V((width, inner), BF16),
        V((2, inner, width), BF16),
        V((width, hidden), BF16), V((width, hidden), BF16), V((hidden, width), BF16),
        V((rows, width), BF16),
        V((rows, inner), BF16), V((rows, inner), BF16), V((rows, inner), BF16),
        V((rows, inner), F32), V((2, rows, inner), BF16),
        V((pairs, 128, 128), BF16),
        V((64 * pairs, 128), F32), V((8, 128), F32), V((64 * pairs, 128), F32), V((8, 128), F32),
        V((8, 128), F32), V((8, 128), F32),
        V((slots, 64 * pairs, 128), BF16), V((slots, 8, 128), F32),
        V((slots, 64 * pairs, 128), BF16), V((slots, 8, 128), F32),
        V((largest, width), F32), V((rows // 2, width), F32),
        halves, halves, early, early,
        V((rows, width), BF16), halves, V((largest, hidden), BF16),
        halves, halves, halves, halves,
        V((inner, rows), BF16), V((rows, heads), F32), V((heads, rows), F32),
        S((8,)), S((CHUNKS,)), S((3,)), S((slots, 3)), S((slots, 3)),
    ] + [S((1,)), S((SUB,))] * 4 + [S((1,)), S((count,)), S((1,)), S((max(PLAIN, 1),))] + [S((1,)), S((count,))] * 3 + [S((1,)), S((count, 2)), S((1,)), S((1,))]
    hbm = pl.BlockSpec(memory_space=pl.ANY)
    vmem = pl.BlockSpec(memory_space=pltpu.VMEM)
    return pl.pallas_call(
        functools.partial(kernel, blocks, steps),
        out_shape=pltpu.VMEM((rows, width), BF16),
        in_specs=[hbm] * 8,
        out_specs=vmem,
        scratch_shapes=scratch,
        compiler_params=pltpu.CompilerParams(
            collective_id=0, has_side_effects=True, vmem_limit_bytes=60_000_000
        ),
    )(
        tokens, forget.T, attn_gain[None, :], projections, out_weight,
        ffn_gain[None, :], expand_weight, down_weight,
    )


def solution(mesh):
    placed = (
        P("seq", None),
        P("seq", "tp"),
        P(),
        P(None, None, "tp"),
        P("tp", None),
        P(),
        P(None, None, "tp"),
        P("tp", None),
    )
    return jax.shard_map(
        functools.partial(local, mesh.shape["seq"]),
        mesh=mesh, in_specs=placed, out_specs=P("seq", None), check_vma=False,
    )
```

```python
import functools

import jax
import jax.numpy as jnp
from jax import lax
from jax.experimental import pallas as pl
from jax.experimental.pallas import tpu as pltpu
from jax.sharding import PartitionSpec as P

norm_epsilon = 1e-05
head_epsilon = 1e-06
MESH = pl.DeviceIdType.MESH
CHUNKS = 4
SIZES = (2, 2, 2, 2)
PLAIN = 1
SUB = 8
FAR_Z = (0,)
FAR_X = (6, 7)
NEAR_Z = (0, 1, 2, 3)
NEAR_X = ()
F32 = jnp.float32
BF16 = jnp.bfloat16


def dot(a, b):
    return jnp.dot(a, b, preferred_element_type=F32)


def contract(a, b, dim_a, dim_b):
    return lax.dot_general(
        a, b, (((dim_a,), (dim_b,)), ((), ())), preferred_element_type=F32
    )


def normalize(widened, gain):
    mean_square = jnp.mean(widened * widened, axis=-1, keepdims=True)
    return (widened * lax.rsqrt(mean_square + norm_epsilon) * gain).astype(BF16)


def kernel(
    blocks, steps,
    tok_hbm, fgt_hbm, again_hbm, proj_hbm, ow_hbm, fgain_hbm, ew_hbm, dw_hbm,
    out,
    fgt, again, fgain,
    tok, wq, wk, wv, wo, wg, wu, wd,
    normed, q, k, v, att, ho, bd, es, el, ts, tl, ed, td, tsb, tsl, trb, trl,
    part, own, dsend1, drecv1, xsend1, xrecv1, nf, res, hid,
    dsend2, drecv2, xsend2, xrecv2,
    ks, ld, ldt,
    wsem, tsem, small_sem, sts, strv, wxs, wxr, wys, wyr, wzs, wzr, wcs, wcr,
    d1s, d1r, x1s, x1r, hs, hr, ns, nr, d2s, d2r, x2s, x2r, osd, orv,
):
    rows, width = tok.shape
    heads = fgt.shape[0]
    inner = wk.shape[1]
    pairs = heads // 2
    chunk = rows // CHUNKS
    me = lax.axis_index("seq")
    tp = lax.axis_index("tp")
    core = lax.rem(tp, 2)
    side = lax.div(tp, 2)
    partner = tp + 1 - 2 * core
    across = lax.rem(tp + 2, 4)
    place = lax.rem(me, 4)
    bit_y = lax.rem(me, 2)
    bit_z = lax.div(place, 2)
    next_y = me + 1 - 2 * bit_y
    next_z = me + 2 - 4 * bit_z

    loads = []
    for at, (src, dst) in enumerate((
        (proj_hbm.at[1], wk), (proj_hbm.at[2], wv), (proj_hbm.at[0], wq),
        (ow_hbm, wo.at[side]), (ew_hbm.at[0], wg), (ew_hbm.at[1], wu), (dw_hbm, wd),
    )):
        copy = pltpu.make_async_copy(src, dst, wsem.at[at])
        loads.append(copy)
    def token_load(r):
        at = pl.ds(pl.multiple_of(r * chunk, chunk), chunk)
        return pltpu.make_async_copy(tok_hbm.at[at], tok.at[at], tsem.at[r])

    small = []
    for at, (src, dst) in enumerate(((fgt_hbm, fgt), (again_hbm, again), (fgain_hbm, fgain))):
        small.append(pltpu.make_async_copy(src, dst, small_sem.at[at]))
    small[0].start()
    for r in range(CHUNKS):
        token_load(r).start()
    small[1].start()
    small[2].start()

    barrier = pltpu.get_barrier_semaphore()
    for other in (partner, across):
        pl.semaphore_signal(barrier, inc=1, device_id={"tp": other}, device_id_type=MESH)
    for other in (next_y, next_z):
        pl.semaphore_signal(barrier, inc=1, device_id={"seq": other}, device_id_type=MESH)
    greeted = 4
    for step in range(1, steps):
        far = 2 ** step
        for reached, other in ((me + far < blocks, me + far), (me >= far, me - far)):
            greeted = greeted + reached.astype(jnp.int32)

            @pl.when(reached)
            def _():
                pl.semaphore_signal(barrier, inc=1, device_id={"seq": other}, device_id_type=MESH)

    quarter = inner // 4
    sub = quarter // SUB

    def strip(owner, j):
        return pl.ds(pl.multiple_of(owner * quarter + j * sub, sub), sub)

    def on_seq(src, dst, ssem, rsem, other):
        return pltpu.make_async_remote_copy(
            src, dst, ssem, rsem, device_id={"seq": other}, device_id_type=MESH)

    def to(src, dst, ssem, rsem, other):
        return pltpu.make_async_remote_copy(
            src, dst, ssem, rsem, device_id={"tp": other}, device_id_type=MESH)

    far_wo = wo.at[1 - side]
    place_y = place + 1 - 2 * bit_y
    place_z = place + 2 - 4 * bit_z

    def wx(j):
        return to(ow_hbm.at[strip(place, j)], wo.at[side, strip(place, j)], wxs.at[0], wxr.at[j], across)

    def wy(j):
        at = strip(place, j)
        return on_seq(far_wo.at[at], far_wo.at[at], wys.at[0], wyr.at[j], next_y)

    def wz(j):
        at = strip(place, j)
        return on_seq(far_wo.at[at], far_wo.at[at], wzs.at[0], wzr.at[j], next_z)

    def wc(j):
        at = strip(3 - place, j)
        return to(ow_hbm.at[at], wo.at[side, at], wcs.at[0], wcr.at[j], across)

    def corner(j, over_z):
        owner, other = (place_y, next_z) if over_z else (place_z, next_y)
        at = strip(owner, j)
        return on_seq(far_wo.at[at], far_wo.at[at], wcs.at[0], wcr.at[j], other)

    far_half = me >= blocks // 2

    def pass_pieces(cond, pieces):
        @pl.when(cond)
        def _():
            for name, j in pieces:
                if "w" in name:
                    wx(j).wait_recv()
                if "y" in name:
                    wy(j).start()
                if "z" in name:
                    wz(j).start()

    near = jnp.logical_not(far_half)

    def by_half(body):
        @pl.when(far_half)
        def _():
            body(FAR_Z, FAR_X)

        @pl.when(near)
        def _():
            body(NEAR_Z, NEAR_X)

    def pass_corners(over_z, straight):
        for j in range(SUB):
            if j in straight:
                continue
            if j in over_z:
                wy(j).wait_recv()
            else:
                wz(j).wait_recv()
            corner(j, j in over_z).start()

    def take_pieces(over_z, straight):
        for j in range(SUB):
            if j in straight or j not in over_z:
                wy(j).wait_recv()
            if j in straight or j in over_z:
                wz(j).wait_recv()
            if j in straight:
                wc(j).wait_recv()
            else:
                corner(j, j in over_z).wait_recv()

    def drain_pieces():
        sent = far_wo.at[pl.ds(pl.multiple_of(place * quarter, quarter), quarter)]
        for sem in (wxs, wys, wzs, wcs):
            to(sent, sent, sem.at[0], wxr.at[0], across).wait_send()

    runs = rows // 128
    tri = (
        lax.broadcasted_iota(jnp.int32, (128, 128), 0)
        <= lax.broadcasted_iota(jnp.int32, (128, 128), 1)
    ).astype(F32).astype(BF16)
    small[0].wait()
    rounded = []
    for b in range(runs):
        left = fgt[:, 128 * b : 128 * b + 128]
        for _ in range(3):
            top = left.astype(BF16).astype(F32)
            rounded.append(top)
            left = left - top
    sums = dot(jnp.concatenate(rounded, axis=0).astype(BF16), tri)
    carried = jnp.zeros((heads, 1), F32)
    for b in range(runs):
        at = 3 * heads * b
        run = sums[at : at + heads] + sums[at + heads : at + 2 * heads]
        run = run + sums[at + 2 * heads : at + 3 * heads] + carried
        ldt[:, 128 * b : 128 * b + 128] = run
        ld[128 * b : 128 * b + 128, :] = run.T
        carried = run[:, 127:128]
    loads[0].start()

    def enter(straight):
        pl.semaphore_wait(barrier, greeted)
        for j in range(SUB):
            wx(j).start()
        for j in straight:
            wc(j).start()

    @pl.when(far_half)
    def _():
        enter(FAR_X)

    def norm_chunk(r, carry):
        at = pl.ds(pl.multiple_of(r * chunk, chunk), chunk)
        token_load(r).wait()
        normed[at, :] = normalize(tok[at, :].astype(F32), again[...])
        return carry

    loads[1].start()
    small[1].wait()
    small[2].wait()
    lax.fori_loop(0, CHUNKS, norm_chunk, 0)

    def project(weight, dst):
        tile = min(256, dst.shape[1])

        def body(j, carry):
            at = pl.ds(pl.multiple_of(j * tile, tile), tile)
            dst[:, at] = dot(normed[...], weight[:, at]).astype(BF16)
            return carry

        lax.fori_loop(0, dst.shape[1] // tile, body, 0)

    loads[2].start()
    loads[3].start()
    loads[0].wait()
    for c in range(2):
        cols = slice(c * (inner // 2), (c + 1) * (inner // 2))
        k[:, cols] = dot(normed[...], wk[:, cols]).astype(BF16)

    @pl.when(near)
    def _():
        enter(NEAR_X)

    loads[1].wait()

    low = lax.broadcasted_iota(jnp.int32, (1, 128), 1) < 64
    low_f = low.astype(F32)
    masks_f = (low_f, 1.0 - low_f)
    masks = (masks_f[0].astype(BF16), masks_f[1].astype(BF16))

    def spread(columns, p):
        return jnp.where(low, columns[:, 2 * p : 2 * p + 1], columns[:, 2 * p + 1 : 2 * p + 2])

    log_decay = ld[...]
    last = log_decay[rows - 1 : rows, :]
    shrink = jnp.exp(ldt[:, rows - 1 : rows] - ldt[...])
    tl[...] = jnp.zeros_like(tl)
    el[...] = jnp.zeros_like(el)
    es[...] = jnp.zeros_like(es)
    for p in range(pairs):
        tl[p : p + 1, :] = spread(last, p)
    part_pairs = pairs // 2

    later = bit_y == 1

    def heir(step):
        return me + 2 ** step if step else next_y

    def sends(step):
        return me + 2 ** step < blocks if step else me >= 0

    def takes(step):
        return me >= 2 ** step if step else me >= 0

    def state_copy(step, part_of):
        at = slice(64 * part_pairs * part_of, 64 * part_pairs * (part_of + 1))
        return pltpu.make_async_remote_copy(
            tsb.at[step, at], trb.at[step, at], sts.at[step, part_of], strv.at[step, part_of],
            device_id={"seq": heir(step)}, device_id_type=MESH)

    def decay_copy(step):
        return pltpu.make_async_remote_copy(
            tsl.at[step], trl.at[step], sts.at[step, 2], strv.at[step, 2],
            device_id={"seq": heir(step)}, device_id_type=MESH)

    def state_copies(step):
        return (decay_copy(step), state_copy(step, 0), state_copy(step, 1))

    def send_state(step, part_of):
        @pl.when(sends(step))
        def _():
            at = slice(64 * part_pairs * part_of, 64 * part_pairs * (part_of + 1))
            if part_of == 0:
                tsl[step] = tl[...]
                decay_copy(step).start()
            tsb[step, at, :] = ts[at, :].astype(BF16)
            state_copy(step, part_of).start()

    def take_state(step):
        for part_of in range(2):
            @pl.when(takes(step))
            def _():
                if part_of == 0:
                    decay_copy(step).wait_recv()
                    ed[...] = jnp.exp(el[...])
                    td[...] = jnp.exp(tl[...])
                    if step == 0:
                        td[...] = jnp.where(later, td[...], jnp.exp(trl[step]))
                        el[...] = jnp.where(later, trl[step], el[...])
                    else:
                        el[...] = el[...] + trl[step]
                    tl[...] = tl[...] + trl[step]
                state_copy(step, part_of).wait_recv()
                for p in range(part_pairs * part_of, part_pairs * (part_of + 1)):
                    at = slice(64 * p, 64 * p + 64)
                    came = trb[step, at, :].astype(F32)
                    decay = td[p : p + 1, :]
                    if step == 0:
                        mine_first = ts[at, :]
                        es[at, :] = jnp.where(later, came, 0.0)
                        ts[at, :] = jnp.where(
                            later, mine_first + decay * came, decay * mine_first + came)
                    else:
                        es[at, :] = es[at, :] + ed[p : p + 1, :] * came
                        ts[at, :] = ts[at, :] + decay * came

            if step + 1 < steps:
                send_state(step + 1, part_of)

    for p in range(pairs):
        turned = k[:, 128 * p : 128 * p + 128].T.astype(F32)
        for j in range(2):
            h = 2 * p + j
            ks[64 * h : 64 * h + 64, :] = (turned[64 * j : 64 * j + 64] * shrink[h : h + 1, :]).astype(BF16)
    each = 128 * part_pairs
    for part_of in range(2):
        cols = slice(each * part_of, each * (part_of + 1))
        v[:, cols] = dot(normed[...], wv[:, cols]).astype(BF16)
        state = dot(ks[cols, :], v[:, cols])
        for p in range(part_pairs):
            at = slice(128 * p, 128 * p + 128)
            pair = state[at, at]
            h = 64 * (part_pairs * part_of + p)
            ts[h : h + 64, :] = pair[:64] * masks_f[0] + pair[64:] * masks_f[1]
        send_state(0, part_of)

    for at in (4, 5, 6):
        loads[at].start()
    loads[2].wait()
    pass_pieces(far_half, (("wz", 0), ("wz", 1)))
    project(wq, q)

    span = rows // 2
    taken = 0
    for p in range(pairs):
        lanes = slice(128 * p, 128 * p + 128)
        for piece in range(2):
            at = slice(piece * span, piece * span + span)
            reach = (piece + 1) * span
            causal = (
                lax.broadcasted_iota(jnp.int32, (span, reach), 0) + piece * span
                >= lax.broadcasted_iota(jnp.int32, (span, reach), 1)
            )
            sums = []
            for j in range(2):
                h = 2 * p + j
                scores = contract(q[at, lanes] * masks[j], k[:reach, lanes], 1, 1)
                gaps = jnp.where(causal, ld[at, h : h + 1] - ldt[h : h + 1, :reach], -1e30)
                weights = (scores * 0.125 * jnp.exp(gaps)).astype(BF16)
                sums.append(dot(weights, v[:reach, lanes]))
            att[at, lanes] = jnp.where(low, sums[0], sums[1])
            if p == 0 and piece:
                pass_pieces(near, (("wy", 0), ("wy", 1)))
            if p % 2 == 0 and piece and taken < steps:
                take_state(taken)
                taken += 1
                if taken == 1:
                    pass_pieces(far_half, (("y", 0), ("y", 1), ("wy", 2)))
                elif taken == 2:
                    pass_pieces(far_half, (("wy", 4),))
                    pass_pieces(near, (("z", 0), ("z", 1), ("z", 2), ("wyz", 3)))
        if p == 1:
            pass_pieces(far_half, (("wy", 3),))
            pass_pieces(near, (("wy", 2),))
        if p == pairs - 1:
            pass_pieces(far_half, (("wy", 5),))
            pass_pieces(near, (("wyz", 4),))
    while taken < steps:
        take_state(taken)
        taken += 1

    pass_pieces(far_half, [("z", j) for j in range(2, 6)] + [("wyz", 6)])

    for p in range(pairs):
        came = es[64 * p : 64 * p + 64, :]
        bd[p] = jnp.concatenate([came * masks_f[0], came * masks_f[1]], axis=0).astype(BF16)
    same_head = (
        (lax.broadcasted_iota(jnp.int32, (128, 128), 0) < 64)
        == (lax.broadcasted_iota(jnp.int32, (128, 128), 1) < 64)
    ).astype(F32).astype(BF16)

    starts, total = [], 0
    for size in SIZES:
        starts.append(total * (rows // sum(SIZES)))
        total += size
    sizes = [size * (rows // sum(SIZES)) for size in SIZES]
    count = len(sizes)

    def whole_rows(r):
        return slice(starts[r], starts[r] + sizes[r])

    def half_rows(r):
        return slice(starts[r] // 2, starts[r] // 2 + sizes[r] // 2)

    def own_rows(r):
        half = sizes[r] // 2
        return pl.ds(pl.multiple_of(starts[r] + core * half, half), half)

    def mine(r):
        half = sizes[r] // 2
        return pl.ds(pl.multiple_of(core * half, half), half)

    def theirs(r):
        half = sizes[r] // 2
        return pl.ds(pl.multiple_of(half - core * half, half), half)

    def d1(r):
        at = half_rows(r)
        return to(dsend1.at[at], drecv1.at[at], d1s.at[0], d1r.at[r], partner)

    def x1(r):
        at = half_rows(r)
        return to(xsend1.at[at], xrecv1.at[at], x1s.at[0], x1r.at[r], across)

    def hx(r):
        at = whole_rows(r)
        return to(ho.at[side, at], ho.at[side, at], hs.at[0], hr.at[r], across)

    def nfc(r):
        return to(nf.at[own_rows(r)], nf.at[own_rows(r)], ns.at[0], nr.at[r], partner)

    def d2(r):
        at = half_rows(r)
        return to(dsend2.at[at], drecv2.at[at], d2s.at[0], d2r.at[r], partner)

    def x2(r, piece):
        n = sizes[r] // 4
        at = pl.ds(starts[r] // 2 + piece * n, n)
        return to(xsend2.at[at], xrecv2.at[at], x2s.at[0], x2r.at[r, piece], across)

    def oc(r, piece):
        at = out_rows(r, piece)
        return to(out.at[at], out.at[at], osd.at[0], orv.at[0], partner)

    def out_rows(r, piece):
        n = sizes[r] // 4
        return pl.ds(pl.multiple_of(starts[r] + core * 2 * n + piece * n, n), n)

    loads[3].wait()
    wide = min(512, width)

    def attend(r):
        at = whole_rows(r)
        reach_decay = jnp.exp(ld[at, :]) * 0.125
        for p in range(pairs):
            lanes = slice(128 * p, 128 * p + 128)
            attended = att[at, lanes] + dot(q[at, lanes], bd[p]) * spread(reach_decay, p)
            mean_square = dot((attended * attended).astype(BF16), same_head) * (1.0 / 64)
            ho[side, at, lanes] = (attended * lax.rsqrt(mean_square + head_epsilon)).astype(BF16)

    def halve(r, send, copy):
        n = sizes[r]
        own[half_rows(r), :] = part[mine(r), :]
        send[half_rows(r), :] = part[theirs(r), :].astype(BF16)
        copy.start()

    def combine(r):
        at, n = whole_rows(r), sizes[r]
        for c in range(width // wide):
            cols = slice(c * wide, c * wide + wide)
            if r < PLAIN:
                part[:n, cols] = dot(ho[side, at, :], wo[side, :, cols])
            else:
                part[:n, cols] = dot(ho[0, at, :], wo[0, :, cols]) + dot(ho[1, at, :], wo[1, :, cols])
        halve(r, dsend1, d1(r))

    def cross(r):
        at = half_rows(r)
        d1(r).wait_recv()
        xsend1[at, :] = (own[at, :] + drecv1[at, :].astype(F32)).astype(BF16)
        x1(r).start()

    def settle(r):
        at = half_rows(r)
        if r < PLAIN:
            x1(r).wait_recv()
            added = xsend1[at, :].astype(F32) + xrecv1[at, :].astype(F32)
        else:
            d1(r).wait_recv()
            added = own[at, :] + drecv1[at, :].astype(F32)
        kept = (tok[own_rows(r), :].astype(F32) + added).astype(BF16)
        res[at, :] = kept
        nf[own_rows(r), :] = normalize(kept.astype(F32), fgain[...])
        nfc(r).start()

    hidden_width = wg.shape[1]
    tile = min(256, hidden_width)

    def forward(r):
        nfc(r).wait_recv()
        at, n = whole_rows(r), sizes[r]
        for c in range(hidden_width // tile):
            cols = slice(c * tile, c * tile + tile)
            gate = dot(nf[at, :], wg[:, cols])
            up = dot(nf[at, :], wu[:, cols])
            hid[:n, cols] = (gate / (1.0 + jnp.exp(-gate)) * up).astype(BF16)
        for c in range(width // wide):
            cols = slice(c * wide, c * wide + wide)
            part[:n, cols] = dot(hid[:n, :], wd[:, cols])
        halve(r, dsend2, d2(r))

    def pass_sums(r):
        at = half_rows(r)
        d2(r).wait_recv()
        xsend2[at, :] = (own[at, :] + drecv2[at, :].astype(F32)).astype(BF16)
        x2(r, 0).start()
        x2(r, 1).start()

    def finish(r, piece):
        n = sizes[r] // 4
        at = slice(starts[r] // 2 + piece * n, starts[r] // 2 + piece * n + n)
        x2(r, piece).wait_recv()
        added = xsend2[at, :].astype(F32) + xrecv2[at, :].astype(F32)
        out[out_rows(r, piece), :] = (res[at, :].astype(F32) + added).astype(BF16)
        oc(r, piece).start()

    if PLAIN < count:
        attend(PLAIN)
        hx(PLAIN).start()
    for r in range(PLAIN):
        attend(r)
        combine(r)
    pass_pieces(far_half, (("wyz", 7),))
    pass_pieces(near, (("wyz", 5),))
    for r in range(PLAIN + 1, count):
        attend(r)
    for r in range(PLAIN):
        cross(r)
    for r in range(PLAIN + 1, count):
        hx(r).start()
    pass_pieces(near, [("wyz", j) for j in range(6, SUB)])
    for at in (4, 5, 6):
        loads[at].wait()

    def arrive():
        by_half(take_pieces)

    def combine_late(r):
        if r == PLAIN:
            arrive()
        hx(r).wait_recv()
        combine(r)

    by_half(pass_corners)
    settle(0)
    for r in range(count):
        if PLAIN < r + 1 < count:
            combine_late(r + 1)
        if r > PLAIN:
            pass_sums(r - 1)
        forward(r)
        if r + 1 == PLAIN < count:
            pl.when(near)(functools.partial(pass_sums, r))
            combine_late(r + 1)
            pl.when(far_half)(functools.partial(pass_sums, r))
        elif r < PLAIN:
            pass_sums(r)
        if r + 1 < count:
            settle(r + 1)
    pass_sums(count - 1)
    drain_pieces()
    for step in range(steps):
        @pl.when(sends(step))
        def _():
            for copy in state_copies(step):
                copy.wait_send()
    to(dsend1, dsend1, d1s.at[0], d1r.at[0], partner).wait_send()
    to(dsend1, dsend1, ns.at[0], nr.at[0], partner).wait_send()
    to(dsend2, dsend2, d2s.at[0], d2r.at[0], partner).wait_send()
    if PLAIN:
        to(xsend1, xsend1, x1s.at[0], x1r.at[0], across).wait_send()
    if PLAIN < count:
        late = ho.at[side, slice(starts[PLAIN], rows)]
        to(late, late, hs.at[0], hr.at[PLAIN], across).wait_send()
    for r in range(count):
        for piece in range(2):
            finish(r, piece)
    to(xsend2, xsend2, x2s.at[0], x2r.at[0, 0], across).wait_send()
    to(xsend2, xrecv2, osd.at[0], orv.at[0], partner).wait()


def local(blocks, tokens, forget, attn_gain, projections, out_weight, ffn_gain, expand_weight, down_weight):
    rows, width = tokens.shape
    heads = forget.shape[1]
    inner = projections.shape[2]
    hidden = down_weight.shape[0]
    pairs = heads // 2
    steps = max(blocks - 1, 0).bit_length()
    V = pltpu.VMEM
    S = pltpu.SemaphoreType.DMA
    slots = max(steps, 1)
    count = len(SIZES)
    largest = rows // sum(SIZES) * max(SIZES)
    halves = V((rows // 2, width), BF16)
    early = V((rows // sum(SIZES) * sum(SIZES[:max(PLAIN, 1)]) // 2, width), BF16)
    scratch = [
        V((heads, rows), F32), V((1, width), F32), V((1, width), F32),
        V((rows, width), BF16),
        V((width, inner), BF16), V((width, inner), BF16), V((width, inner), BF16),
        V((2, inner, width), BF16),
        V((width, hidden), BF16), V((width, hidden), BF16), V((hidden, width), BF16),
        V((rows, width), BF16),
        V((rows, inner), BF16), V((rows, inner), BF16), V((rows, inner), BF16),
        V((rows, inner), F32), V((2, rows, inner), BF16),
        V((pairs, 128, 128), BF16),
        V((64 * pairs, 128), F32), V((8, 128), F32), V((64 * pairs, 128), F32), V((8, 128), F32),
        V((8, 128), F32), V((8, 128), F32),
        V((slots, 64 * pairs, 128), BF16), V((slots, 8, 128), F32),
        V((slots, 64 * pairs, 128), BF16), V((slots, 8, 128), F32),
        V((largest, width), F32), V((rows // 2, width), F32),
        halves, halves, early, early,
        V((rows, width), BF16), halves, V((largest, hidden), BF16),
        halves, halves, halves, halves,
        V((inner, rows), BF16), V((rows, heads), F32), V((heads, rows), F32),
        S((8,)), S((CHUNKS,)), S((3,)), S((slots, 3)), S((slots, 3)),
    ] + [S((1,)), S((SUB,))] * 4 + [S((1,)), S((count,)), S((1,)), S((max(PLAIN, 1),))] + [S((1,)), S((count,))] * 3 + [S((1,)), S((count, 2)), S((1,)), S((1,))]
    hbm = pl.BlockSpec(memory_space=pl.ANY)
    vmem = pl.BlockSpec(memory_space=pltpu.VMEM)
    return pl.pallas_call(
        functools.partial(kernel, blocks, steps),
        out_shape=pltpu.VMEM((rows, width), BF16),
        in_specs=[hbm] * 8,
        out_specs=vmem,
        scratch_shapes=scratch,
        compiler_params=pltpu.CompilerParams(
            collective_id=0, has_side_effects=True, vmem_limit_bytes=60_000_000
        ),
    )(
        tokens, forget.T, attn_gain[None, :], projections, out_weight,
        ffn_gain[None, :], expand_weight, down_weight,
    )


def solution(mesh):
    placed = (
        P("seq", None),
        P("seq", "tp"),
        P(),
        P(None, None, "tp"),
        P("tp", None),
        P(),
        P(None, None, "tp"),
        P("tp", None),
    )
    return jax.shard_map(
        functools.partial(local, mesh.shape["seq"]),
        mesh=mesh, in_specs=placed, out_specs=P("seq", None), check_vma=False,
    )
```
